32 devices in a mesh: rep: 1, dp: 32 (over x, y, z, core).
Axes of the slice: x: 2, y: 2, z: 4, core: 2. Of those that a mesh axis runs over, the one named last changes fastest.
Arguments:
- x: bfloat16 [32, 2048, 1024], P(('rep', 'dp'))
- dy: bfloat16 [32, 2048, 1024], P(('rep', 'dp'))
- w_gate: bfloat16 [2, 1024, 3200], P(None, 'dp')
- w_up: bfloat16 [2, 1024, 3200], P(None, 'dp')
- w_down: bfloat16 [2, 3200, 1024], P(None, 'dp')
- m_w_gate: float32 [2, 1024, 3200], P(None, 'dp')
- m_w_up: float32 [2, 1024, 3200], P(None, 'dp')
- m_w_down: float32 [2, 3200, 1024], P(None, 'dp')
- v_w_gate: float32 [2, 1024, 3200], P(None, 'dp')
- v_w_up: float32 [2, 1024, 3200], P(None, 'dp')
- v_w_down: float32 [2, 3200, 1024], P(None, 'dp')
Outputs:
- output 1: bfloat16 [2, 1024, 3200], P('rep', 'dp')
- output 2: bfloat16 [2, 1024, 3200], P('rep', 'dp')
- output 3: bfloat16 [2, 3200, 1024], P('rep', 'dp')
- output 4: float32 [2, 1024, 3200], P('rep', 'dp')
- output 5: float32 [2, 1024, 3200], P('rep', 'dp')
- output 6: float32 [2, 3200, 1024], P('rep', 'dp')
- output 7: float32 [2, 1024, 3200], P('rep', 'dp')
- output 8: float32 [2, 1024, 3200], P('rep', 'dp')
- output 9: float32 [2, 3200, 1024], P('rep', 'dp')
All inputs are finite; a program needn't handle non-finite values.
Results may differ from the reference program's by a relative error of at most 0.0279.
Values are sent between devices in bfloat16 or wider.
A program may use at most 2 GiB of HBM per device.

```python
import jax
import jax.numpy as jnp
from jax import lax

SEQUENCES = 32
TOKENS = 2048
D = 1024
FF = 3200
LAYERS = 2
NAMES = ("w_gate", "w_up", "w_down")
SHAPES = {"w_gate": (LAYERS, D, FF), "w_up": (LAYERS, D, FF), "w_down": (LAYERS, FF, D)}


def bump(key, n, height):
    away = (jnp.arange(n, dtype=jnp.int32) - jax.random.randint(key, (), 0, n, jnp.int32)) % n
    return jnp.where(away < n // 8, height, 1.0)


def together(key, own, strength):
    shared = jax.random.normal(key, own.shape[1:], jnp.float32)
    return (own + strength * shared) * lax.rsqrt(1 + strength * strength)


def setup_inputs(seed: int = 0, part: int = 0) -> dict:
    kx, kdy, ka, kb, kz, kf, kh, kl, *keys = jax.random.split(jax.random.key(seed), 8 + 3 * len(NAMES))
    kx, kdy, ka, kb = (jax.random.fold_in(k, part) for k in (kx, kdy, ka, kb))
    kw, km, kv = (keys[i::3] for i in range(3))
    shape = (SEQUENCES, TOKENS, D)
    much_x, much_dy = jax.random.uniform(kz, (2,), jnp.float32, 0.0, 1.0)
    loud = 2.0 ** jax.random.uniform(jax.random.fold_in(kz, 1), (), jnp.float32, -1.0, 2.0)
    layers = 2.0 ** jax.random.uniform(kl, (LAYERS, 1, 1), jnp.float32, -1.0, 1.0)
    x = together(ka, jax.random.normal(kx, shape, jnp.float32), much_x) * bump(kf, D, 4.0)
    dy = together(kb, jax.random.normal(kdy, shape, jnp.float32), much_dy)
    drawn = {"x": x.astype(jnp.bfloat16), "dy": (loud * dy * (SEQUENCES * TOKENS) ** -0.5).astype(jnp.bfloat16)}
    for key, name in zip(kw, NAMES, strict=True):
        w = jax.random.normal(key, SHAPES[name], jnp.float32) * SHAPES[name][1] ** -0.5
        drawn[name] = (w * {"w_gate": 1.0, "w_up": bump(kh, FF, 4.0), "w_down": layers}[name]).astype(jnp.bfloat16)
    for key, name in zip(km, NAMES, strict=True):
        drawn[f"m_{name}"] = 0.1 * jax.random.normal(key, SHAPES[name], jnp.float32)
    for key, name in zip(kv, NAMES, strict=True):
        drawn[f"v_{name}"] = jax.random.uniform(key, SHAPES[name], jnp.float32, 0.005, 0.015)
    return drawn


def matmul(a, w):
    return jnp.dot(a, w, preferred_element_type=jnp.float32).astype(jnp.bfloat16)


def normed(h):
    wide = h.astype(jnp.float32)
    scale = lax.rsqrt(jnp.mean(wide**2, -1, keepdims=True) + 1e-6)
    return (wide * scale).astype(jnp.bfloat16)


def layer(h, w):
    a = normed(h)
    gate = jnp.dot(a, w["w_gate"], preferred_element_type=jnp.float32)
    up = jnp.dot(a, w["w_up"], preferred_element_type=jnp.float32)
    return h + matmul((jax.nn.silu(gate) * up).astype(jnp.bfloat16), w["w_down"])


def adamw(w, m, v, g):
    m = 0.9 * m + 0.1 * g
    v = 0.95 * v + 0.05 * g * g
    step = m * lax.rsqrt(v + 1e-8) + 0.1 * w
    return (w - 0.02 * step).astype(jnp.bfloat16), m, v


def clipped(gradients, sum_of_squares, count):
    factor = jnp.minimum(1.0, 0.5 * lax.rsqrt(sum_of_squares / count + 1e-30))
    return [g * factor for g in gradients]


def stack(weights, h):
    return lax.scan(lambda h, w: (layer(h, w), None), h, weights)[0]


def reference(x, dy, w_gate, w_up, w_down, m_w_gate, m_w_up, m_w_down, v_w_gate, v_w_up, v_w_down):
    weights = dict(zip(NAMES, (w_gate, w_up, w_down), strict=True))

    def take(so_far, sequence):
        h, by_y = sequence
        _, back = jax.vjp(lambda w: stack(w, h), weights)
        return jax.tree.map(lambda total, term: total + term.astype(jnp.float32), so_far, back(by_y)[0]), None

    none_yet = {name: jnp.zeros(w.shape, jnp.float32) for name, w in weights.items()}
    by_weights, _ = lax.scan(take, none_yet, (x, dy))
    gradients = [by_weights[name].astype(jnp.bfloat16).astype(jnp.float32) for name in NAMES]
    gradients = clipped(gradients, sum(jnp.sum(g * g) for g in gradients), sum(g.size for g in gradients))
    new = [
        adamw(w.astype(jnp.float32), m, v, g)
        for w, m, v, g in zip((w_gate, w_up, w_down), (m_w_gate, m_w_up, m_w_down), (v_w_gate, v_w_up, v_w_down), gradients, strict=True)
    ]
    return tuple(one[which] for which in range(3) for one in new)
```

```python
import jax
import jax.numpy as jnp
from jax import lax
from jax.experimental import pallas as pl
from jax.experimental.pallas import tpu as pltpu
from jax.sharding import PartitionSpec as P

T, D, F = 2048, 1024, 3200
BF, F32 = jnp.bfloat16, jnp.float32
ANY = pl.BlockSpec(memory_space=pl.ANY)
NT = (((1,), (1,)), ((), ()))
TN = (((0,), (0,)), ((), ()))

X, Y, ZH, ZL, C = 16, 8, 4, 2, 1
R = {X: 2, Y: 1}


def normed(h):
    wide = h.astype(F32)
    scale = lax.rsqrt(jnp.mean(wide**2, -1, keepdims=True) + 1e-6)
    return (wide * scale).astype(BF)


def cost(flops, moved, trans=0):
    return pl.CostEstimate(flops=flops, bytes_accessed=moved, transcendentals=trans)


def peer(bits):
    index = lax.axis_index("dp")
    there = index
    for bit in (X, Y, ZH, ZL, C):
        if bits & bit:
            there = there + bit - 2 * bit * ((index // bit) % 2)
    return there


def at_peer(bits, low, high):
    return (peer(bits) // low) % (2 * high // low)


class Gather:
    def __init__(self, own, shape, rounds, steps, home):
        self.home = home
        self.ins, self.outs, self.rounds, self.steps = [own], [jax.ShapeDtypeStruct(shape, BF)], rounds, steps
        self.scratch = [pltpu.VMEM(own.shape, BF), pltpu.SemaphoreType.DMA]

    def place(self, ins, outs, scratch):
        staged, sem = scratch
        dst = self.home(outs[0])
        for pair in ((ins[0], staged), (staged, dst)):
            copy = pltpu.make_async_copy(*pair, sem)
            copy.start()
            copy.wait()


def wide_gather(own, first, second, steps):
    a, b = R[first], R[second]

    def rounds(ins, outs):
        (own,), (buf,) = ins, outs
        part = lambda r, k: buf.at[r, k]
        return [
            [(own, buf.at[0, 0, at_peer(0, ZL, ZH)], 2 * j) for j in (1, 2, 3)],
            [(part(0, 0), part(a, 0), first), (part(0, 0), part(b, 0), second), (part(0, 0), part(0, 1), C)],
            [(part(a, 0), part(3, 0), second), (part(a, 0), part(a, 1), C), (part(b, 0), part(b, 1), C)],
            [(part(3, 0), part(3, 1), C)],
        ]

    return Gather(own, (4, 2, 4, 32, F), rounds, steps, lambda buf: buf.at[0, 0, at_peer(0, ZL, ZH)])


def down_gather(own, first, second, steps):
    a, b = R[first], R[second]

    def rounds(ins, outs):
        (own,), (buf,) = ins, outs
        part = lambda l, k, r: buf.at[l, k, r]
        across = lambda l, *rs: [(part(l, 0, r), part(l, 1, r), C) for r in rs]
        over = lambda *rs: [(part(0, 0, r), part(1, 0, r), ZL) for r in rs]
        return [
            [(own, buf.at[0, 0, 0, at_peer(0, ZH, ZH)], ZH)],
            [(part(0, 0, 0), part(0, 0, a), first), (part(0, 0, 0), part(0, 0, b), second)] + over(0) + across(0, 0),
            [(part(0, 0, a), part(0, 0, 3), second)] + over(a, b) + across(0, a, b) + across(1, 0),
            over(3) + across(0, 3) + across(1, a, b),
            across(1, 3),
        ]

    return Gather(own, (2, 2, 4, 2, 400, 256), rounds, steps, lambda buf: buf.at[0, 0, 0, at_peer(0, ZH, ZH)])


class Swap:
    def __init__(self, *pairs, step=0):
        self.ins = [a for a, _ in pairs]
        self.outs = [jax.ShapeDtypeStruct(a.shape, a.dtype) for a in self.ins]
        self.rounds = lambda ins, outs: [[(s, d, bits) for s, d, (_, bits) in zip(ins, outs, pairs)]]
        self.steps, self.scratch = [step], []

    def place(self, ins, outs, scratch):
        pass


class Finish(Swap):
    def __init__(self, parts, first, second, steps):
        self.ins, self.steps, self.scratch = [parts[first], parts[second]], steps, []
        self.outs = [jax.ShapeDtypeStruct((4, 32, F), BF)] * 4
        self.rounds = lambda i, o: [[(i[0], o[0], second), (i[0], o[1], C), (i[1], o[2], C)], [(o[0], o[3], C)]]


def run(body, comms, *, grid, ins, in_specs, outs, out_specs, scratch, number, name, estimate=None):
    n_in, n_out, n_scratch = len(ins), len(outs), len(scratch)
    counts = [(len(c.ins), len(c.outs), len(c.scratch)) for c in comms]
    total = 1
    for n in grid:
        total *= n

    def take(refs, which, start):
        found, at = [], start
        for count in counts:
            found.append(refs[at : at + count[which]])
            at += count[which]
        return found, at

    def kernel(*refs):
        mine_in = refs[:n_in]
        their_ins, at = take(refs, 0, n_in)
        mine_out, at = refs[at : at + n_out], at + n_out
        their_outs, at = take(refs, 1, at)
        mine_scratch, at = refs[at : at + n_scratch], at + n_scratch
        their_scratch, at = take(refs, 2, at)
        send, recv = refs[at:] if comms else (None, None)
        copies, used, bits = [], 0, []
        for c, i, o in zip(comms, their_ins, their_outs):
            per = []
            for one in c.rounds(i, o):
                here = []
                for source, target, b in one:
                    here.append((source, target, b, used))
                    used += 1
                    if b not in bits:
                        bits.append(b)
                per.append(here)
            copies.append(per)

        def make(item):
            source, target, b, n = item
            return pltpu.make_async_remote_copy(
                src_ref=source, dst_ref=target, send_sem=send.at[n], recv_sem=recv.at[n],
                device_id={"dp": peer(b)}, device_id_type=pl.DeviceIdType.MESH,
            )

        events = sorted((s, n, p) for p, c in enumerate(comms) for n, s in enumerate(c.steps))
        if not grid:
            step = 0
        else:
            step = pl.program_id(0)
            for d in range(1, len(grid)):
                step = step * grid[d] + pl.program_id(d)

        def enter():
            barrier = pltpu.get_barrier_semaphore()
            for b in bits:
                pl.semaphore_signal(barrier, inc=1, device_id={"dp": peer(b)}, device_id_type=pl.DeviceIdType.MESH)
            for c, i, o, s in zip(comms, their_ins, their_outs, their_scratch):
                c.place(i, o, s)
            pl.semaphore_wait(barrier, len(bits))

        def advance(now):
            for s, n, p in events:
                if s == now:
                    if n:
                        for item in copies[p][n - 1]:
                            make(item).wait()
                    for item in copies[p][n]:
                        make(item).start()

        def leave():
            for p, c in enumerate(comms):
                for item in copies[p][-1]:
                    make(item).wait()

        if not comms:
            return body(mine_in, mine_out, mine_scratch)
        times = sorted({s for s, _, _ in events})
        if not grid:
            enter()
            for t in times:
                advance(t)
            leave()
            return
        for t in times:

            @pl.when(step == t)
            def _():
                if t == 0:
                    enter()
                advance(t)

        body(mine_in, mine_out, mine_scratch)

        @pl.when(step == total - 1)
        def _():
            leave()

    n_copies = 0
    for c in comms:
        fake = lambda shapes: [Shape(s.shape) for s in shapes]
        n_copies += sum(len(one) for one in c.rounds(fake(c.ins), fake(c.outs)))
    all_scratch = list(scratch) + [s for c in comms for s in c.scratch]
    if comms:
        all_scratch += [pltpu.SemaphoreType.DMA((n_copies,))] * 2
    n_comm_in, n_comm_out = sum(c[0] for c in counts), sum(c[1] for c in counts)
    call = pl.pallas_call(
        kernel,
        grid=grid,
        in_specs=list(in_specs) + [ANY] * n_comm_in,
        out_specs=list(out_specs) + [ANY] * n_comm_out,
        out_shape=list(outs) + [s for c in comms for s in c.outs],
        scratch_shapes=all_scratch,
        compiler_params=pltpu.CompilerParams(collective_id=number, has_side_effects=True) if comms else pltpu.CompilerParams(),
        cost_estimate=estimate,
        name=name,
    )
    return call, (*ins, *[a for c in comms for a in c.ins])


class Shape:
    def __init__(self, shape):
        self.shape, self.at = shape, self

    def __getitem__(self, _):
        return self


def wide_copies(pieces, slot, sem, columns, place):
    for r in range(4):
        for k in range(2):
            piece = pieces[2 * r + k] if len(pieces) == 8 else pieces[0].at[r, k]
            yield pltpu.make_async_copy(piece.at[:, :, columns], slot.at[at_peer(r * Y, Y, X), :, at_peer(k, C, C), :, place], sem)


def down_copies(pieces, slot, sem):
    for l in range(2):
        for k in range(2):
            columns = pl.ds(pl.multiple_of(at_peer(l * ZL + k, C, ZL) * 256, 256), 256)
            for r in range(4):
                yield pltpu.make_async_copy(pieces.at[l, k, r], slot.at[at_peer(r * Y, Y, X), :, :, columns], sem)


def struct(shape, dtype=BF):
    return jax.ShapeDtypeStruct(shape, dtype)


def gate_up(a, gate_w, up_w, comms, number):
    blocks, chunks, rows = 5, 5, 512

    def body(ins, outs, scratch):
        a_ref, *w_refs = ins
        g_ref, u_ref = w_refs[: len(gate_w)], w_refs[len(gate_w) :]
        act_ref, s_ref, t_ref = outs
        slots, sems = scratch
        n, m = pl.program_id(0), pl.program_id(1)

        def copies(block, slot):
            start = pl.multiple_of(block * chunks * 128, 128)
            for k, pieces in enumerate((g_ref, u_ref)):
                yield from wide_copies(pieces, slots.at[slot, k], sems.at[slot], pl.ds(start, chunks * 128), slice(None))

        now = n % 2

        @pl.when((n == 0) & (m == 0))
        def _():
            for copy in copies(0, 0):
                copy.start()

        @pl.when(m == 0)
        def _():
            for copy in copies(n, now):
                copy.wait()

            @pl.when(n + 1 < blocks)
            def _():
                for copy in copies(n + 1, 1 - now):
                    copy.start()

        lhs = a_ref[...]
        for i in range(chunks):
            w = jnp.concatenate([slots[now, k, :, :, :, :, i * 128 : i * 128 + 128].reshape(D, 128) for k in range(2)], 1)
            both = jnp.dot(lhs, w, preferred_element_type=F32)
            gate, up = both[:, :128], both[:, 128:]
            sig = 1.0 / (1.0 + jnp.exp(-gate))
            s = gate * sig
            at = slice(i * 128, i * 128 + 128)
            act_ref[:, at] = (s * up).astype(BF)
            s_ref[:, at] = s
            t_ref[:, at] = up * (sig + s * (1.0 - sig))

    out = pl.BlockSpec((rows, chunks * 128), lambda n, m: (m, n))
    call, operands = run(
        body, comms, grid=(blocks, T // rows),
        ins=[a, *gate_w, *up_w], in_specs=[pl.BlockSpec((rows, D), lambda n, m: (m, 0))] + [ANY] * len(gate_w + up_w),
        outs=[struct((T, F)), struct((T, F), F32), struct((T, F), F32)], out_specs=[out] * 3,
        scratch=[pltpu.VMEM((2, 2, 4, 4, 2, 32, chunks * 128), BF), pltpu.SemaphoreType.DMA((2,))],
        number=number, name="gate_up", estimate=cost(4 * T * D * F, T * F * 10 + 4 * D * F, T * F * 2),
    )
    return call(*operands)


def row(rows, n):
    return pl.BlockSpec((rows, n), lambda m: (m, 0))


def fetch_down(p_ref, w_ref, sem):
    @pl.when(pl.program_id(0) == 0)
    def _():
        for copy in down_copies(p_ref, w_ref, sem):
            copy.start()
        for copy in down_copies(p_ref, w_ref, sem):
            copy.wait()


def down(act, h, pieces, comms, number):
    def body(ins, outs, scratch):
        act_ref, h_ref, p_ref = ins
        fetch_down(p_ref, *scratch)
        out = h_ref[...] + jnp.dot(act_ref[...], scratch[0][...].reshape(F, D), preferred_element_type=F32).astype(BF)
        outs[0][...] = out
        outs[1][...] = normed(out)

    call, operands = run(
        body, comms, grid=(T // 256,), ins=[act, h, pieces], in_specs=[row(256, F), row(256, D), ANY],
        outs=[struct((T, D))] * 2, out_specs=[row(256, D)] * 2, scratch=[pltpu.VMEM((4, 2, 400, D), BF), pltpu.SemaphoreType.DMA],
        number=number, name="down", estimate=cost(2 * T * D * F, T * F * 2 + T * D * 6 + 2 * D * F),
    )
    return call(*operands)


def by_hidden(dh, s, t, pieces, comms, number):
    def body(ins, outs, scratch):
        dh_ref, s_ref, t_ref, p_ref = ins
        dg_ref, du_ref = outs
        w_ref = scratch[0]
        fetch_down(p_ref, *scratch)
        lhs = dh_ref[...]
        w = w_ref[...].reshape(F, D)
        for at in range(0, F, 640):
            at = slice(at, at + 640)
            d = lax.dot_general(lhs, w[at, :], NT, preferred_element_type=F32).astype(BF).astype(F32)
            du_ref[:, at] = (d * s_ref[:, at]).astype(BF)
            dg_ref[:, at] = (d * t_ref[:, at]).astype(BF)

    call, operands = run(
        body, comms, grid=(T // 256,), ins=[dh, s, t, pieces], in_specs=[row(256, D), row(256, F), row(256, F), ANY],
        outs=[struct((T, F))] * 2, out_specs=[row(256, F)] * 2, scratch=[pltpu.VMEM((4, 2, 400, D), BF), pltpu.SemaphoreType.DMA],
        number=number, name="by_hidden", estimate=cost(2 * T * D * F, T * F * 12 + T * D * 2 + 2 * D * F),
    )
    return call(*operands)


def by_input(dg, du, dh, h, gate_w, up_w, comms, number):
    def body(ins, outs, scratch):
        dg_ref, du_ref, dh_ref, h_ref, *w_refs = ins
        g_ref, u_ref = w_refs[: len(gate_w)], w_refs[len(gate_w) :]
        slots, sems = scratch

        @pl.when(pl.program_id(0) == 0)
        def _():
            both = [c for k, p in enumerate((g_ref, u_ref)) for c in wide_copies(p, slots.at[k], sems.at[k], slice(None), slice(None))]
            for copy in both:
                copy.start()
            for copy in both:
                copy.wait()

        halves = []
        for k, d_ref in enumerate((dg_ref, du_ref)):
            w = slots[k].reshape(D, F)
            halves.append(lax.dot_general(d_ref[...], w, NT, preferred_element_type=F32).astype(BF))
        da = (halves[0] + halves[1]).astype(F32)
        wide = h_ref[...].astype(F32)
        scale = lax.rsqrt(jnp.mean(wide**2, -1, keepdims=True) + 1e-6)
        along = jnp.mean(da * wide, -1, keepdims=True)
        outs[0][...] = dh_ref[...] + (da * scale - wide * (scale * scale * scale * along)).astype(BF)

    call, operands = run(
        body, comms, grid=(T // 256,), ins=[dg, du, dh, h, *gate_w, *up_w],
        in_specs=[row(256, F), row(256, F), row(256, D), row(256, D)] + [ANY] * len(gate_w + up_w),
        outs=[struct((T, D))], out_specs=[row(256, D)],
        scratch=[pltpu.VMEM((2, 4, 4, 2, 32, F), BF), pltpu.SemaphoreType.DMA((2,))],
        number=number, name="by_input", estimate=cost(4 * T * D * F, T * F * 4 + T * D * 6 + 4 * D * F),
    )
    return call(*operands)


def by_wide(at, d, comms, number):
    columns = 640

    def body(ins, outs, scratch):
        at_ref, d_ref = ins
        for k, ref in enumerate(outs):
            ref[...] = jnp.dot(at_ref[k * D // 2 : (k + 1) * D // 2, :], d_ref[...], preferred_element_type=F32).astype(BF)

    out = pl.BlockSpec((D // 2, columns), lambda n: (0, n))
    call, operands = run(
        body, comms, grid=(F // columns,), ins=[at, d],
        in_specs=[pl.BlockSpec((D, T), lambda n: (0, 0)), pl.BlockSpec((T, columns), lambda n: (0, n))],
        outs=[struct((D // 2, F))] * 2, out_specs=[out] * 2, scratch=[],
        number=number, name="by_wide", estimate=cost(2 * T * D * F, T * F * 2 + T * D * 2 + D * F * 2),
    )
    return call(*operands)


def by_down(act, dh, comms, number):
    rows = 640

    def body(ins, outs, scratch):
        act_ref, dh_ref = ins
        for n, ref in enumerate(outs):
            columns = pl.ds(pl.multiple_of(at_peer(n, C, ZL) * 256, 256), 256)
            ref[...] = lax.dot_general(act_ref[...], dh_ref[:, columns], TN, preferred_element_type=F32).astype(BF)

    call, operands = run(
        body, comms, grid=(F // rows,), ins=[act, dh],
        in_specs=[pl.BlockSpec((T, rows), lambda n: (0, n)), pl.BlockSpec((T, D), lambda n: (0, 0))],
        outs=[struct((F, 256))] * 4, out_specs=[pl.BlockSpec((rows, 256), lambda n: (n, 0))] * 4, scratch=[],
        number=number, name="by_down", estimate=cost(2 * T * D * F, T * F * 2 + T * D * 2 + D * F * 2),
    )
    return call(*operands)


def only(comms, number, name):
    call, operands = run(None, comms, grid=(), ins=[], in_specs=[], outs=[], out_specs=[], scratch=[], number=number, name=name)
    return call(*operands)


def everyone(value, number):
    groups = (tuple(range(1, 8)), (8, 16, 24))

    def kernel(value_ref, out_ref, mid_ref, slots, send, recv):
        barrier = pltpu.get_barrier_semaphore()
        for b in groups[0] + groups[1]:
            pl.semaphore_signal(barrier, inc=1, device_id={"dp": peer(b)}, device_id_type=pl.DeviceIdType.MESH)
        pl.semaphore_wait(barrier, 10)
        source, target, n = value_ref, mid_ref, 0
        for group in groups:
            copies = []
            for b in group:
                copies.append(
                    pltpu.make_async_remote_copy(
                        src_ref=source, dst_ref=slots.at[n], send_sem=send.at[n], recv_sem=recv.at[n],
                        device_id={"dp": peer(b)}, device_id_type=pl.DeviceIdType.MESH,
                    )
                )
                copies[-1].start()
                n += 1
            total = source[...]
            for i, copy in enumerate(copies):
                copy.wait()
                total = total + slots[n - len(copies) + i]
            target[...] = total
            source, target = mid_ref, out_ref

    spec = pl.BlockSpec(memory_space=pltpu.VMEM)
    return pl.pallas_call(
        kernel, in_specs=[spec], out_specs=spec, out_shape=struct((8, 128), F32),
        scratch_shapes=[pltpu.VMEM((8, 128), F32), pltpu.VMEM((10, 8, 128), F32)] + [pltpu.SemaphoreType.DMA((10,))] * 2,
        compiler_params=pltpu.CompilerParams(collective_id=number, has_side_effects=True), name="everyone",
    )(jnp.broadcast_to(value, (8, 128)))[0, 0]


def adamw(w, m, v, g):
    m = 0.9 * m + 0.1 * g
    v = 0.95 * v + 0.05 * g * g
    step = m * lax.rsqrt(v + 1e-8) + 0.1 * w
    return (w - 0.02 * step).astype(BF), m, v


def f32(a):
    return a.astype(F32)


LEFT, RIGHT = slice(0, 1664), slice(1664, F)


class WideSum:
    def __init__(self, keep, send):
        self.keep, self.send = keep.reshape(4, 4, 32, F), send.reshape(4, 4, 32, F)

    def core(self):
        return [(self.send, C)]

    def got_core(self, got):
        self.pair = lambda r, columns: f32(self.keep[r][..., columns]) + f32(got[r][..., columns])

    def axis(self):
        one = lambda r, columns: self.pair(r, columns).astype(BF)
        return [(one(3, LEFT), X), (one(2, LEFT), X), (one(3, RIGHT), Y), (one(1, RIGHT), Y)]

    def got_axis(self, *got):
        self.got = got

    def other(self):
        return [((self.pair(1, LEFT) + f32(self.got[0])).astype(BF), Y), ((self.pair(2, RIGHT) + f32(self.got[2])).astype(BF), X)]

    def got_other(self, left, right):
        self.left = self.pair(0, LEFT) + f32(self.got[1]) + f32(left)
        self.right = self.pair(0, RIGHT) + f32(self.got[3]) + f32(right)

    def z(self):
        return [(side[j].astype(BF), 2 * j) for side in (self.left, self.right) for j in (1, 2, 3)]

    def got_z(self, *rest):
        total = lambda side, some: (side[0] + sum(f32(r) for r in some)).astype(BF)
        self.sum = jnp.concatenate([total(self.left, rest[:3]), total(self.right, rest[3:])], 1)


class DownSum:
    def __init__(self, parts, spot):
        self.parts, self.spot = parts, spot

    def core(self):
        return [(self.parts[1], C), (self.parts[3], C)]

    def got_core(self, mine, low):
        self.mine = mine
        self.to_low = (f32(self.parts[2]) + f32(low)).astype(BF).reshape(2, 1600, 256)

    def low(self, n):
        return [(self.to_low[n], ZL)]

    def got_low(self, *got):
        q = self.spot[0]
        quarters = lambda a: a.reshape(4, 2, 400, 256)
        pick = lambda a, r, side: f32(lax.dynamic_index_in_dim(quarters(a), r ^ q, 0, False)[side])

        def lows(r, side):
            both = [g.reshape(2, 2, 400, 256) for g in got]
            at = r ^ q
            return f32(jnp.where(at < 2, *[lax.dynamic_index_in_dim(b, at & 1, 0, False)[side] for b in both]))

        self.pair = lambda r, side: pick(self.parts[0], r, side) + pick(self.mine, r, side) + lows(r, side)

    def axis(self):
        one = lambda r, side: self.pair(r, side).astype(BF)
        return [(one(3, 0), X), (one(2, 0), X), (one(3, 1), Y), (one(1, 1), Y)]

    def got_axis(self, *got):
        self.got = got

    def other(self):
        return [((self.pair(1, 0) + f32(self.got[0])).astype(BF), Y), ((self.pair(2, 1) + f32(self.got[2])).astype(BF), X)]

    def got_other(self, first, second):
        total = jnp.stack([self.pair(0, 0) + f32(self.got[1]) + f32(first), self.pair(0, 1) + f32(self.got[3]) + f32(second)])
        self.half = lambda h: lax.dynamic_index_in_dim(total, h ^ self.spot[1], 0, False)

    def high(self):
        return [(self.half(1).astype(BF), ZH)]

    def got_high(self, got):
        self.block = (self.half(0) + f32(got)).astype(BF).reshape(4, 100, 256)

    def rows(self):
        pick = lambda n: lax.dynamic_index_in_dim(self.block, n ^ self.spot[2], 0, False)
        self.own = pick(0)
        return [(pick(n), n) for n in (1, 2, 3)]

    def got_rows(self, *rest):
        stacked = jnp.stack((self.own,) + rest)
        self.sum = jnp.concatenate([lax.dynamic_index_in_dim(stacked, n ^ self.spot[2], 0, False) for n in range(4)], 1)


def solution(mesh):
    def step(x, dy, *arrays):
        weights, m, v = (arrays[i : i + 3] for i in (0, 3, 6))
        index = lax.axis_index("dp")
        q, zh, p = index >> 3, (index >> 2) & 1, index & 3
        z, c = (index >> 1) & 3, index & 1
        spot = (q, zh, p)
        ids = iter(range(100))

        columns = weights[2].reshape(2, 100, 4, 256).transpose(2, 0, 1, 3)
        part = lambda n: lax.dynamic_index_in_dim(columns, n ^ p, 0, False)
        h0, dh = x[0], dy[0]
        a0 = normed(h0)
        own_g, own_u = weights[0][1], weights[1][1]
        g0, u0, t1, t2, t3, *along = only(
            [
                wide_gather(weights[0][0], X, Y, [0, 2, 4, 6]),
                wide_gather(weights[1][0], Y, X, [1, 3, 5, 7]),
                Swap(*[(part(n), n) for n in (1, 2, 3)], step=1),
                Swap(*[(w, 2 * n) for w in (own_g, own_u) for n in (1, 2, 3)], step=3),
            ],
            next(ids), "fetch",
        )
        ordered = lambda parts, me: jnp.stack([lax.dynamic_index_in_dim(jnp.stack(parts), n ^ me, 0, False) for n in range(len(parts))])
        line_g, line_u = ordered([own_g, *along[:3]], z), ordered([own_u, *along[3:]], z)
        stacked = jnp.stack([part(0), t1, t2, t3])
        turned_down = jnp.concatenate([lax.dynamic_index_in_dim(stacked, n ^ p, 0, False) for n in range(4)], 1)

        at = jnp.arange(D)
        k, r, j, i = at >> 9, (at >> 7) & 3, (at >> 5) & 3, at & 31
        source = (r ^ q) * 256 + (j ^ z) * 64 + (k ^ c) * 32 + i
        order = (source[:, None] == jnp.arange(D)[None, :]).astype(BF)
        turned = lambda a: jnp.einsum("pk,tk->pt", order, a, preferred_element_type=F32).astype(BF)

        act0, s0, t0, d0, gx, gy, gc, uy, ux, uc = gate_up(
            a0, [g0], [u0],
            [
                down_gather(turned_down[0], X, Y, [0, 4, 11, 15, 19]),
                Swap((line_g, X), (line_g, Y), (line_g, C), step=0),
                Swap((line_u, Y), (line_u, X), (line_u, C), step=12),
            ],
            next(ids),
        )
        h1, a1, g3, gxc, gyc, g3c, u3, uyc, uxc, u3c = down(
            act0, h0, d0, [Finish({X: gx, Y: gy}, X, Y, [0, 7]), Finish({X: ux, Y: uy}, Y, X, [0, 7])], next(ids)
        )
        g1 = [line_g, gc, gy, gyc, gx, gxc, g3, g3c]
        u1 = [line_u, uc, uy, uyc, ux, uxc, u3, u3c]
        at0, at1 = turned(a0), turned(a1)
        act1, s1, t1, d1 = gate_up(a1, g1, u1, [down_gather(turned_down[1], Y, X, [0, 4, 8, 15, 19])], next(ids))

        def under(kernel, *args, n, during, name=None):
            pairs = [send() for send, _ in during]
            flat = [pair for some in pairs for pair in some]
            comms = [Swap(*flat)] if flat else []
            out = list(kernel(*args, comms, next(ids)) if name is None else only(comms, next(ids), name))
            at = n
            for some, (_, give) in zip(pairs, during):
                give(*out[at : at + len(some)])
                at += len(some)
            return out[:n]

        lows = {}

        def low(one, n):
            def got(a):
                lows.setdefault(one, []).append(a)
                if n:
                    one.got_low(*lows[one])

            return (lambda: one.low(n)), got

        go = lambda one, name: (getattr(one, name), getattr(one, "got_" + name))
        D1 = DownSum(under(by_down, act1, dh, n=4, during=[]), spot)
        dg, du = under(by_hidden, dh, s1, t1, d1, n=2, during=[go(D1, "core")])
        G1 = WideSum(*under(by_wide, at1, dg, n=2, during=[low(D1, 0)]))
        U1 = WideSum(*under(by_wide, at1, du, n=2, during=[low(D1, 1), go(G1, "core")]))
        (dh,) = under(by_input, dg, du, dh, h1, g1, u1, n=1, during=[go(G1, "axis"), go(U1, "core"), go(D1, "axis")])
        D0 = DownSum(under(by_down, act0, dh, n=4, during=[go(G1, "other"), go(U1, "axis")]), spot)
        dg, du = under(by_hidden, dh, s0, t0, d0, n=2, during=[go(D0, "core"), go(G1, "z"), go(U1, "other"), go(D1, "other")])
        G0 = WideSum(*under(by_wide, at0, dg, n=2, during=[low(D0, 0), go(D1, "high")]))
        U0 = WideSum(*under(by_wide, at0, du, n=2, during=[low(D0, 1), go(G0, "core"), go(D1, "rows")]))
        under(None, n=0, name="tail_1", during=[go(U0, "core"), go(G0, "axis"), go(U1, "z"), go(D0, "axis")])
        under(None, n=0, name="tail_2", during=[go(U0, "axis"), go(G0, "other"), go(D0, "other")])
        under(None, n=0, name="tail_3", during=[go(U0, "other"), go(G0, "z"), go(D0, "high")])
        under(None, n=0, name="tail_4", during=[go(U0, "z"), go(D0, "rows")])

        sums = [[f32(one.sum) for one in layer] for layer in ((G0, U0, D0), (G1, U1, D1))]
        squares = everyone(sum(jnp.sum(g * g) for layer in sums for g in layer), next(ids))
        factor = jnp.minimum(1.0, 0.5 * lax.rsqrt(squares / (6 * D * F) + 1e-30))
        new = []
        for i in range(3):
            g = jnp.stack([sums[0][i], sums[1][i]]) * factor
            new.append(adamw(weights[i].astype(F32), m[i], v[i], g))
        return tuple(one[which] for which in range(3) for one in new)

    states, cut = P(("rep", "dp"), None, None), P(None, "dp", None)
    return jax.shard_map(
        step,
        mesh=mesh,
        in_specs=(states, states) + (cut,) * 9,
        out_specs=(P("rep", "dp", None),) * 9,
        check_vma=False,
    )
```

```python
import jax
import jax.numpy as jnp
from jax import lax
from jax.experimental import pallas as pl
from jax.experimental.pallas import tpu as pltpu
from jax.sharding import PartitionSpec as P

T, D, F = 2048, 1024, 3200
BF, F32 = jnp.bfloat16, jnp.float32
ANY = pl.BlockSpec(memory_space=pl.ANY)
NT = (((1,), (1,)), ((), ()))
TN = (((0,), (0,)), ((), ()))

X, Y, ZH, ZL, C = 16, 8, 4, 2, 1
R = {X: 2, Y: 1}


def normed(h):
    wide = h.astype(F32)
    scale = lax.rsqrt(jnp.mean(wide**2, -1, keepdims=True) + 1e-6)
    return (wide * scale).astype(BF)


def cost(flops, moved, trans=0):
    return pl.CostEstimate(flops=flops, bytes_accessed=moved, transcendentals=trans)


def peer(bits):
    index = lax.axis_index("dp")
    there = index
    for bit in (X, Y, ZH, ZL, C):
        if bits & bit:
            there = there + bit - 2 * bit * ((index // bit) % 2)
    return there


def at_peer(bits, low, high):
    return (peer(bits) // low) % (2 * high // low)


class Gather:
    def __init__(self, own, shape, rounds, steps, home):
        self.home = home
        self.ins, self.outs, self.rounds, self.steps = [own], [jax.ShapeDtypeStruct(shape, BF)], rounds, steps
        self.scratch = [pltpu.VMEM(own.shape, BF), pltpu.SemaphoreType.DMA]

    def place(self, ins, outs, scratch):
        staged, sem = scratch
        dst = self.home(outs[0])
        for pair in ((ins[0], staged), (staged, dst)):
            copy = pltpu.make_async_copy(*pair, sem)
            copy.start()
            copy.wait()


def wide_gather(own, first, second, steps):
    a, b = R[first], R[second]

    def rounds(ins, outs):
        (own,), (buf,) = ins, outs
        part = lambda r, k: buf.at[r, k]
        here = at_peer(0, ZL, ZH)
        there = [at_peer(2 * j, ZL, ZH) for j in (1, 2, 3)]
        over = lambda r, bit: [(buf.at[0, 0, j], buf.at[r, 0, j], bit) for j in there]
        return [
            [(own, buf.at[0, 0, here], 2 * j) for j in (1, 2, 3)] + [(own, buf.at[a, 0, here], first), (own, buf.at[b, 0, here], second)],
            over(a, first) + over(b, second) + [(part(0, 0), part(0, 1), C)],
            [(part(a, 0), part(3, 0), second), (part(a, 0), part(a, 1), C), (part(b, 0), part(b, 1), C)],
            [(part(3, 0), part(3, 1), C)],
        ]

    return Gather(own, (4, 2, 4, 32, F), rounds, steps, lambda buf: buf.at[0, 0, at_peer(0, ZL, ZH)])


def down_gather(own, first, second, steps):
    lined = len(own.shape) == 3
    a, b = R[first], R[second]

    def rounds(ins, outs):
        (own,), (buf,) = ins, outs
        part = lambda l, k, r: buf.at[l, k, r]
        across = lambda l, *rs: [(part(l, 0, r), part(l, 1, r), C) for r in rs]
        over = lambda *rs: [(part(0, 0, r), part(1, 0, r), ZL) for r in rs]
        start = [] if lined else [[(own, buf.at[0, 0, 0, at_peer(0, ZH, ZH)], ZH)]]
        return start + [
            [(part(0, 0, 0), part(0, 0, a), first), (part(0, 0, 0), part(0, 0, b), second)] + over(0) + across(0, 0),
            [(part(0, 0, a), part(0, 0, 3), second)] + over(a, b) + across(0, a, b) + across(1, 0),
            over(3) + across(0, 3) + across(1, a, b),
            across(1, 3),
        ]

    return Gather(own, (2, 2, 4, 2, 400, 256), rounds, steps, lambda buf: buf.at[0, 0, 0] if lined else buf.at[0, 0, 0, at_peer(0, ZH, ZH)])


class Swap:
    def __init__(self, *pairs, step=0):
        self.ins = [a for a, _ in pairs]
        self.outs = [jax.ShapeDtypeStruct(a.shape, a.dtype) for a in self.ins]
        self.rounds = lambda ins, outs: [[(s, d, bits) for s, d, (_, bits) in zip(ins, outs, pairs)]]
        self.steps, self.scratch = [step], []

    def place(self, ins, outs, scratch):
        pass


class Halves(Swap):
    def __init__(self, line, first, second, steps):
        self.ins, self.steps, self.scratch = [line], steps, []
        self.outs = [jax.ShapeDtypeStruct(line.shape, BF)] * 3
        self.rounds = lambda i, o: [
            [(i[0].at[:2], o[0].at[:2], first), (i[0].at[:2], o[1].at[:2], second)],
            [(i[0].at[2:], o[0].at[2:], first), (i[0].at[2:], o[1].at[2:], second), (i[0], o[2], C)],
        ]


class Finish(Swap):
    def __init__(self, parts, first, second, steps):
        self.ins, self.steps, self.scratch = [parts[first], parts[second]], steps, []
        self.outs = [jax.ShapeDtypeStruct((4, 32, F), BF)] * 4
        self.rounds = lambda i, o: [[(i[0], o[0], second), (i[0], o[1], C), (i[1], o[2], C)], [(o[0], o[3], C)]]


def run(body, comms, *, grid, ins, in_specs, outs, out_specs, scratch, number, name, estimate=None):
    n_in, n_out, n_scratch = len(ins), len(outs), len(scratch)
    counts = [(len(c.ins), len(c.outs), len(c.scratch)) for c in comms]
    total = 1
    for n in grid:
        total *= n

    def take(refs, which, start):
        found, at = [], start
        for count in counts:
            found.append(refs[at : at + count[which]])
            at += count[which]
        return found, at

    def kernel(*refs):
        mine_in = refs[:n_in]
        their_ins, at = take(refs, 0, n_in)
        mine_out, at = refs[at : at + n_out], at + n_out
        their_outs, at = take(refs, 1, at)
        mine_scratch, at = refs[at : at + n_scratch], at + n_scratch
        their_scratch, at = take(refs, 2, at)
        send, recv = refs[at:] if comms else (None, None)
        copies, used, bits = [], 0, []
        for c, i, o in zip(comms, their_ins, their_outs):
            per = []
            for one in c.rounds(i, o):
                here = []
                for source, target, b in one:
                    here.append((source, target, b, used))
                    used += 1
                    if b not in bits:
                        bits.append(b)
                per.append(here)
            copies.append(per)

        def make(item):
            source, target, b, n = item
            return pltpu.make_async_remote_copy(
                src_ref=source, dst_ref=target, send_sem=send.at[n], recv_sem=recv.at[n],
                device_id={"dp": peer(b)}, device_id_type=pl.DeviceIdType.MESH,
            )

        events = sorted((s, n, p) for p, c in enumerate(comms) for n, s in enumerate(c.steps))
        if not grid:
            step = 0
        else:
            step = pl.program_id(0)
            for d in range(1, len(grid)):
                step = step * grid[d] + pl.program_id(d)

        def enter():
            barrier = pltpu.get_barrier_semaphore()
            for b in bits:
                pl.semaphore_signal(barrier, inc=1, device_id={"dp": peer(b)}, device_id_type=pl.DeviceIdType.MESH)
            for c, i, o, s in zip(comms, their_ins, their_outs, their_scratch):
                c.place(i, o, s)
            pl.semaphore_wait(barrier, len(bits))

        def advance(now):
            for s, n, p in events:
                if s == now:
                    if n:
                        for item in copies[p][n - 1]:
                            make(item).wait()
                    for item in copies[p][n]:
                        make(item).start()

        def leave():
            for p, c in enumerate(comms):
                for item in copies[p][-1]:
                    make(item).wait()

        if not comms:
            return body(mine_in, mine_out, mine_scratch)
        times = sorted({s for s, _, _ in events})
        if not grid:
            enter()
            for t in times:
                advance(t)
            leave()
            return
        for t in times:

            @pl.when(step == t)
            def _():
                if t == 0:
                    enter()
                advance(t)

        body(mine_in, mine_out, mine_scratch)

        @pl.when(step == total - 1)
        def _():
            leave()

    n_copies = 0
    for c in comms:
        fake = lambda shapes: [Shape(s.shape) for s in shapes]
        n_copies += sum(len(one) for one in c.rounds(fake(c.ins), fake(c.outs)))
    all_scratch = list(scratch) + [s for c in comms for s in c.scratch]
    if comms:
        all_scratch += [pltpu.SemaphoreType.DMA((n_copies,))] * 2
    n_comm_in, n_comm_out = sum(c[0] for c in counts), sum(c[1] for c in counts)
    call = pl.pallas_call(
        kernel,
        grid=grid,
        in_specs=list(in_specs) + [ANY] * n_comm_in,
        out_specs=list(out_specs) + [ANY] * n_comm_out,
        out_shape=list(outs) + [s for c in comms for s in c.outs],
        scratch_shapes=all_scratch,
        compiler_params=pltpu.CompilerParams(collective_id=number, has_side_effects=True) if comms else pltpu.CompilerParams(),
        cost_estimate=estimate,
        name=name,
    )
    return call, (*ins, *[a for c in comms for a in c.ins])


class Shape:
    def __init__(self, shape):
        self.shape, self.at = shape, self

    def __getitem__(self, _):
        return self


def wide_copies(pieces, slot, sem, columns, place):
    for r in range(4):
        for k in range(2):
            piece = pieces[2 * r + k] if len(pieces) == 8 else pieces[0].at[r, k]
            yield pltpu.make_async_copy(piece.at[:, :, columns], slot.at[at_peer(r * Y, Y, X), :, at_peer(k, C, C), :, place], sem)


def down_copies(pieces, slot, sem):
    for l in range(2):
        for k in range(2):
            columns = pl.ds(pl.multiple_of(at_peer(l * ZL + k, C, ZL) * 256, 256), 256)
            for r in range(4):
                yield pltpu.make_async_copy(pieces.at[l, k, r], slot.at[at_peer(r * Y, Y, X), :, :, columns], sem)


def struct(shape, dtype=BF):
    return jax.ShapeDtypeStruct(shape, dtype)


def gate_up(a, gate_w, up_w, comms, number):
    blocks, chunks, rows = 5, 5, 512

    def body(ins, outs, scratch):
        a_ref, *w_refs = ins
        g_ref, u_ref = w_refs[: len(gate_w)], w_refs[len(gate_w) :]
        act_ref, s_ref, t_ref = outs
        slots, sems = scratch
        n, m = pl.program_id(0), pl.program_id(1)

        def copies(block, slot):
            start = pl.multiple_of(block * chunks * 128, 128)
            for k, pieces in enumerate((g_ref, u_ref)):
                yield from wide_copies(pieces, slots.at[slot, k], sems.at[slot], pl.ds(start, chunks * 128), slice(None))

        now = n % 2

        @pl.when((n == 0) & (m == 0))
        def _():
            for copy in copies(0, 0):
                copy.start()

        @pl.when(m == 0)
        def _():
            for copy in copies(n, now):
                copy.wait()

            @pl.when(n + 1 < blocks)
            def _():
                for copy in copies(n + 1, 1 - now):
                    copy.start()

        lhs = a_ref[...]
        for i in range(chunks):
            w = jnp.concatenate([slots[now, k, :, :, :, :, i * 128 : i * 128 + 128].reshape(D, 128) for k in range(2)], 1)
            both = jnp.dot(lhs, w, preferred_element_type=F32)
            gate, up = both[:, :128], both[:, 128:]
            sig = 1.0 / (1.0 + jnp.exp(-gate))
            s = gate * sig
            at = slice(i * 128, i * 128 + 128)
            act_ref[:, at] = (s * up).astype(BF)
            s_ref[:, at] = s
            t_ref[:, at] = up * (sig + s * (1.0 - sig))

    out = pl.BlockSpec((rows, chunks * 128), lambda n, m: (m, n))
    call, operands = run(
        body, comms, grid=(blocks, T // rows),
        ins=[a, *gate_w, *up_w], in_specs=[pl.BlockSpec((rows, D), lambda n, m: (m, 0))] + [ANY] * len(gate_w + up_w),
        outs=[struct((T, F)), struct((T, F), F32), struct((T, F), F32)], out_specs=[out] * 3,
        scratch=[pltpu.VMEM((2, 2, 4, 4, 2, 32, chunks * 128), BF), pltpu.SemaphoreType.DMA((2,))],
        number=number, name="gate_up", estimate=cost(4 * T * D * F, T * F * 10 + 4 * D * F, T * F * 2),
    )
    return call(*operands)


def row(rows, n):
    return pl.BlockSpec((rows, n), lambda m: (m, 0))


def fetch_down(p_ref, w_ref, sem):
    @pl.when(pl.program_id(0) == 0)
    def _():
        for copy in down_copies(p_ref, w_ref, sem):
            copy.start()
        for copy in down_copies(p_ref, w_ref, sem):
            copy.wait()


def down(act, h, pieces, comms, number):
    def body(ins, outs, scratch):
        act_ref, h_ref, p_ref = ins
        fetch_down(p_ref, *scratch)
        out = h_ref[...] + jnp.dot(act_ref[...], scratch[0][...].reshape(F, D), preferred_element_type=F32).astype(BF)
        outs[0][...] = out
        outs[1][...] = normed(out)

    call, operands = run(
        body, comms, grid=(T // 256,), ins=[act, h, pieces], in_specs=[row(256, F), row(256, D), ANY],
        outs=[struct((T, D))] * 2, out_specs=[row(256, D)] * 2, scratch=[pltpu.VMEM((4, 2, 400, D), BF), pltpu.SemaphoreType.DMA],
        number=number, name="down", estimate=cost(2 * T * D * F, T * F * 2 + T * D * 6 + 2 * D * F),
    )
    return call(*operands)


def by_hidden(dh, s, t, pieces, comms, number):
    def body(ins, outs, scratch):
        dh_ref, s_ref, t_ref, p_ref = ins
        dg_ref, du_ref = outs
        w_ref = scratch[0]
        fetch_down(p_ref, *scratch)
        lhs = dh_ref[...]
        w = w_ref[...].reshape(F, D)
        for at in range(0, F, 640):
            at = slice(at, at + 640)
            d = lax.dot_general(lhs, w[at, :], NT, preferred_element_type=F32).astype(BF).astype(F32)
            du_ref[:, at] = (d * s_ref[:, at]).astype(BF)
            dg_ref[:, at] = (d * t_ref[:, at]).astype(BF)

    call, operands = run(
        body, comms, grid=(T // 256,), ins=[dh, s, t, pieces], in_specs=[row(256, D), row(256, F), row(256, F), ANY],
        outs=[struct((T, F))] * 2, out_specs=[row(256, F)] * 2, scratch=[pltpu.VMEM((4, 2, 400, D), BF), pltpu.SemaphoreType.DMA],
        number=number, name="by_hidden", estimate=cost(2 * T * D * F, T * F * 12 + T * D * 2 + 2 * D * F),
    )
    return call(*operands)


def by_input(dg, du, dh, h, gate_w, up_w, comms, number):
    def body(ins, outs, scratch):
        dg_ref, du_ref, dh_ref, h_ref, *w_refs = ins
        g_ref, u_ref = w_refs[: len(gate_w)], w_refs[len(gate_w) :]
        slots, sems = scratch

        @pl.when(pl.program_id(0) == 0)
        def _():
            both = [c for k, p in enumerate((g_ref, u_ref)) for c in wide_copies(p, slots.at[k], sems.at[k], slice(None), slice(None))]
            for copy in both:
                copy.start()
            for copy in both:
                copy.wait()

        halves = []
        for k, d_ref in enumerate((dg_ref, du_ref)):
            w = slots[k].reshape(D, F)
            halves.append(lax.dot_general(d_ref[...], w, NT, preferred_element_type=F32).astype(BF))
        da = (halves[0] + halves[1]).astype(F32)
        wide = h_ref[...].astype(F32)
        scale = lax.rsqrt(jnp.mean(wide**2, -1, keepdims=True) + 1e-6)
        along = jnp.mean(da * wide, -1, keepdims=True)
        outs[0][...] = dh_ref[...] + (da * scale - wide * (scale * scale * scale * along)).astype(BF)

    call, operands = run(
        body, comms, grid=(T // 256,), ins=[dg, du, dh, h, *gate_w, *up_w],
        in_specs=[row(256, F), row(256, F), row(256, D), row(256, D)] + [ANY] * len(gate_w + up_w),
        outs=[struct((T, D))], out_specs=[row(256, D)],
        scratch=[pltpu.VMEM((2, 4, 4, 2, 32, F), BF), pltpu.SemaphoreType.DMA((2,))],
        number=number, name="by_input", estimate=cost(4 * T * D * F, T * F * 4 + T * D * 6 + 4 * D * F),
    )
    return call(*operands)


def by_wide(at, d, comms, number):
    columns = 640

    def body(ins, outs, scratch):
        at_ref, d_ref = ins
        for k, ref in enumerate(outs):
            ref[...] = jnp.dot(at_ref[k * D // 2 : (k + 1) * D // 2, :], d_ref[...], preferred_element_type=F32).astype(BF)

    out = pl.BlockSpec((D // 2, columns), lambda n: (0, n))
    call, operands = run(
        body, comms, grid=(F // columns,), ins=[at, d],
        in_specs=[pl.BlockSpec((D, T), lambda n: (0, 0)), pl.BlockSpec((T, columns), lambda n: (0, n))],
        outs=[struct((D // 2, F))] * 2, out_specs=[out] * 2, scratch=[],
        number=number, name="by_wide", estimate=cost(2 * T * D * F, T * F * 2 + T * D * 2 + D * F * 2),
    )
    return call(*operands)


def by_down(act, dh, comms, number):
    rows = 640

    def body(ins, outs, scratch):
        act_ref, dh_ref = ins
        for n, ref in enumerate(outs):
            columns = pl.ds(pl.multiple_of(at_peer(n, C, ZL) * 256, 256), 256)
            ref[...] = lax.dot_general(act_ref[...], dh_ref[:, columns], TN, preferred_element_type=F32).astype(BF)

    call, operands = run(
        body, comms, grid=(F // rows,), ins=[act, dh],
        in_specs=[pl.BlockSpec((T, rows), lambda n: (0, n)), pl.BlockSpec((T, D), lambda n: (0, 0))],
        outs=[struct((F, 256))] * 4, out_specs=[pl.BlockSpec((rows, 256), lambda n: (n, 0))] * 4, scratch=[],
        number=number, name="by_down", estimate=cost(2 * T * D * F, T * F * 2 + T * D * 2 + D * F * 2),
    )
    return call(*operands)


def only(comms, number, name):
    call, operands = run(None, comms, grid=(), ins=[], in_specs=[], outs=[], out_specs=[], scratch=[], number=number, name=name)
    return call(*operands)


class Copies:
    def __init__(self, send, recv):
        self.send, self.recv, self.n = send, recv, 0

    def __call__(self, source, target, bits):
        copy = pltpu.make_async_remote_copy(
            src_ref=source, dst_ref=target, send_sem=self.send.at[self.n], recv_sem=self.recv.at[self.n],
            device_id={"dp": peer(bits)}, device_id_type=pl.DeviceIdType.MESH,
        )
        copy.start()
        self.n += 1
        return copy


def meet(bits):
    barrier = pltpu.get_barrier_semaphore()
    for b in bits:
        pl.semaphore_signal(barrier, inc=1, device_id={"dp": peer(b)}, device_id_type=pl.DeviceIdType.MESH)
    pl.semaphore_wait(barrier, len(bits))


VMEM = pl.BlockSpec(memory_space=pltpu.VMEM)


def everyone(value, pieces, number):
    groups = (tuple(range(1, 8)), (8, 16, 24))

    def kernel(value_ref, p1, p2, p3, out_ref, o1, o2, o3, mid_ref, slots, send, recv):
        meet(groups[0] + groups[1])
        begin = Copies(send, recv)
        source, target, n = value_ref, mid_ref, 0
        rest = []
        for group in groups:
            copies = [begin(source, slots.at[n + i], b) for i, b in enumerate(group)]
            if not rest:
                rest = [begin(a, b, bits) for a, b, bits in ((p1, o1, 1), (p2, o2, 2), (p3, o3, 3))]
            total = source[...]
            for copy in copies:
                copy.wait()
                total = total + slots[n]
                n += 1
            target[...] = total
            source, target = mid_ref, out_ref
        for copy in rest:
            copy.wait()

    call = pl.pallas_call(
        kernel, in_specs=[VMEM] + [ANY] * 3, out_specs=[VMEM] + [ANY] * 3,
        out_shape=[struct((8, 128), F32)] + [struct(a.shape) for a in pieces],
        scratch_shapes=[pltpu.VMEM((8, 128), F32), pltpu.VMEM((10, 8, 128), F32)] + [pltpu.SemaphoreType.DMA((13,))] * 2,
        compiler_params=pltpu.CompilerParams(collective_id=number, has_side_effects=True), name="everyone",
    )
    total, *got = call(jnp.broadcast_to(value, (8, 128)), *pieces)
    return total[0, 0], got


def tail(wides, pair, swaps, number):
    n, width, ns = 5, 640, len(swaps)
    ways = ((X, Y), (Y, X))

    def kernel(*refs):
        keeps, sends, pd = refs[:2], refs[2:4], refs[4]
        swap_in, refs = refs[5 : 5 + ns], refs[5 + ns :]
        outs, out_d, swap_out, refs = refs[:2], refs[2], refs[3 : 3 + ns], refs[3 + ns :]
        got, snd1, rcv1, snd2, rcv2, tot, snd3, rcv3, sd1, rd1, sd2, rd2, td, sd3, rd3, send, recv = refs
        begin = Copies(send, recv)
        at = lambda u: slice(u * width, (u + 1) * width)
        meet((C, X, Y, 2, 4, 6))
        core = [[begin(sends[w].at[:, at(u)], got.at[w, u], C) for w in range(2)] for u in range(n)]
        others = [begin(a, b, bits) for a, b, (_, bits) in zip(swap_in, swap_out, swaps)]
        first, second, last, down1, down2, down3 = {}, {}, {}, {}, {}, []

        def term(w, u, r):
            rows = slice(r * 128, r * 128 + 128)
            return f32(keeps[w][rows, at(u)]) + f32(got[w, u, rows, :])

        def axis(u):
            for w, (one, _) in enumerate(ways):
                core[u][w].wait()
                snd1[w, u, 0] = term(w, u, 3).astype(BF)
                snd1[w, u, 1] = term(w, u, R[one]).astype(BF)
            for i in range(2):
                for w, (one, _) in enumerate(ways):
                    first[w, u, i] = begin(snd1.at[w, u, i], rcv1.at[w, u, i], one)

        def other(u):
            for w, (_, two) in enumerate(ways):
                first[w, u, 0].wait()
                snd2[w, u] = (term(w, u, R[two]) + f32(rcv1[w, u, 0])).astype(BF)
            for w, (_, two) in enumerate(ways):
                second[w, u] = begin(snd2.at[w, u], rcv2.at[w, u], two)

        def line(u):
            for w in range(2):
                first[w, u, 1].wait()
                second[w, u].wait()
                total = term(w, u, 0) + f32(rcv1[w, u, 1]) + f32(rcv2[w, u])
                tot[w, u] = total[:32]
                for j in (1, 2, 3):
                    snd3[w, u, j - 1] = total[32 * j : 32 * j + 32].astype(BF)
            for w in range(2):
                last[w, u] = [begin(snd3.at[w, u, j - 1], rcv3.at[w, u, j - 1], 2 * j) for j in (1, 2, 3)]

        def end(u):
            for w in range(2):
                total = tot[w, u]
                for i, copy in enumerate(last[w, u]):
                    copy.wait()
                    total = total + f32(rcv3[w, u, i])
                outs[w][:, at(u)] = total.astype(BF)

        def down_axis():
            for w, (one, _) in enumerate(ways):
                sd1[w, 0] = pd[3, w].astype(BF)
                sd1[w, 1] = pd[R[one], w].astype(BF)
            for w, (one, _) in enumerate(ways):
                down1[w] = [begin(sd1.at[w, i], rd1.at[w, i], one) for i in range(2)]

        def down_other():
            for w, (_, two) in enumerate(ways):
                down1[w][0].wait()
                sd2[w] = (pd[R[two], w] + f32(rd1[w, 0])).astype(BF)
            for w, (_, two) in enumerate(ways):
                down2[w] = begin(sd2.at[w], rd2.at[w], two)

        def down_line():
            for w in range(2):
                down1[w][1].wait()
                down2[w].wait()
                td[w] = pd[0, w] + f32(rd1[w, 1]) + f32(rd2[w])
            sd3[...] = td[at_peer(ZH, ZH, ZH)].astype(BF)
            down3.append(begin(sd3, rd3, ZH))

        for s in range(n + 3):
            if s < n:
                axis(s)
            if s == 1:
                down_axis()
            if 0 <= s - 1 < n:
                other(s - 1)
            if s == 3:
                down_other()
            if 0 <= s - 2 < n:
                line(s - 2)
            if s == 4:
                down_line()
            if 0 <= s - 3 < n:
                end(s - 3)
        down3[0].wait()
        out_d[...] = (td[at_peer(0, ZH, ZH)] + f32(rd3[...])).astype(BF)
        for copy in others:
            copy.wait()

    vm = lambda *shape: pltpu.VMEM(shape, BF)
    total = n * 2 * 7 + 7 + ns
    call = pl.pallas_call(
        kernel, in_specs=[VMEM] * 2 + [ANY] * 2 + [VMEM] + [ANY] * ns, out_specs=[VMEM] * 3 + [ANY] * ns,
        out_shape=[struct((32, F))] * 2 + [struct((400, 256))] + [struct(a.shape) for a, _ in swaps],
        scratch_shapes=[
            vm(2, n, 512, width), vm(2, n, 2, 128, width), vm(2, n, 2, 128, width), vm(2, n, 128, width), vm(2, n, 128, width),
            pltpu.VMEM((2, n, 32, width), F32), vm(2, n, 3, 32, width), vm(2, n, 3, 32, width),
            vm(2, 2, 400, 256), vm(2, 2, 400, 256), vm(2, 400, 256), vm(2, 400, 256), pltpu.VMEM((2, 400, 256), F32), vm(400, 256), vm(400, 256),
        ] + [pltpu.SemaphoreType.DMA((total,))] * 2,
        compiler_params=pltpu.CompilerParams(collective_id=number, has_side_effects=True), name="tail",
    )
    return call(*[w.keep.reshape(512, F) for w in wides], *[w.send.reshape(512, F) for w in wides], pair, *[a for a, _ in swaps])


def adamw(w, m, v, g):
    m = 0.9 * m + 0.1 * g
    v = 0.95 * v + 0.05 * g * g
    step = m * lax.rsqrt(v + 1e-8) + 0.1 * w
    return (w - 0.02 * step).astype(BF), m, v


def f32(a):
    return a.astype(F32)


LEFT, RIGHT = slice(0, 1664), slice(1664, F)


class WideSum:
    def __init__(self, keep, send):
        self.keep, self.send = keep.reshape(4, 4, 32, F), send.reshape(4, 4, 32, F)

    def core(self):
        return [(self.send, C)]

    def got_core(self, got):
        self.pair = lambda r, columns: f32(self.keep[r][..., columns]) + f32(got[r][..., columns])

    def axis(self):
        one = lambda r, columns: self.pair(r, columns).astype(BF)
        return [(one(3, LEFT), X), (one(2, LEFT), X), (one(3, RIGHT), Y), (one(1, RIGHT), Y)]

    def got_axis(self, *got):
        self.got = got

    def other(self):
        return [((self.pair(1, LEFT) + f32(self.got[0])).astype(BF), Y), ((self.pair(2, RIGHT) + f32(self.got[2])).astype(BF), X)]

    def got_other(self, left, right):
        self.left = self.pair(0, LEFT) + f32(self.got[1]) + f32(left)
        self.right = self.pair(0, RIGHT) + f32(self.got[3]) + f32(right)

    def z(self):
        return [(side[j].astype(BF), 2 * j) for side in (self.left, self.right) for j in (1, 2, 3)]

    def got_z(self, *rest):
        total = lambda side, some: (side[0] + sum(f32(r) for r in some)).astype(BF)
        self.sum = jnp.concatenate([total(self.left, rest[:3]), total(self.right, rest[3:])], 1)


class DownSum:
    def __init__(self, parts, spot):
        self.parts, self.spot = parts, spot

    def core(self):
        return [(self.parts[1], C), (self.parts[3], C)]

    def got_core(self, mine, low):
        self.mine = mine
        self.to_low = (f32(self.parts[2]) + f32(low)).astype(BF).reshape(2, 1600, 256)

    def low(self, n):
        return [(self.to_low[n], ZL)]

    def got_low(self, *got):
        q = self.spot[0]
        quarters = lambda a: a.reshape(4, 2, 400, 256)
        pick = lambda a, r, side: f32(lax.dynamic_index_in_dim(quarters(a), r ^ q, 0, False)[side])

        def lows(r, side):
            both = [g.reshape(2, 2, 400, 256) for g in got]
            at = r ^ q
            return f32(jnp.where(at < 2, *[lax.dynamic_index_in_dim(b, at & 1, 0, False)[side] for b in both]))

        self.pair = lambda r, side: pick(self.parts[0], r, side) + pick(self.mine, r, side) + lows(r, side)

    def axis(self):
        one = lambda r, side: self.pair(r, side).astype(BF)
        return [(one(3, 0), X), (one(2, 0), X), (one(3, 1), Y), (one(1, 1), Y)]

    def got_axis(self, *got):
        self.got = got

    def other(self):
        return [((self.pair(1, 0) + f32(self.got[0])).astype(BF), Y), ((self.pair(2, 1) + f32(self.got[2])).astype(BF), X)]

    def got_other(self, first, second):
        total = jnp.stack([self.pair(0, 0) + f32(self.got[1]) + f32(first), self.pair(0, 1) + f32(self.got[3]) + f32(second)])
        self.half = lambda h: lax.dynamic_index_in_dim(total, h ^ self.spot[1], 0, False)

    def high(self):
        return [(self.half(1).astype(BF), ZH)]

    def got_high(self, got):
        self.block = (self.half(0) + f32(got)).astype(BF).reshape(4, 100, 256)

    def rows(self):
        pick = lambda n: lax.dynamic_index_in_dim(self.block, n ^ self.spot[2], 0, False)
        self.own = pick(0)
        return [(pick(n), n) for n in (1, 2, 3)]

    def got_rows(self, *rest):
        stacked = jnp.stack((self.own,) + rest)
        self.sum = jnp.concatenate([lax.dynamic_index_in_dim(stacked, n ^ self.spot[2], 0, False) for n in range(4)], 1)


def solution(mesh):
    def step(x, dy, *arrays):
        weights, m, v = (arrays[i : i + 3] for i in (0, 3, 6))
        index = lax.axis_index("dp")
        q, zh, p = index >> 3, (index >> 2) & 1, index & 3
        z, c = (index >> 1) & 3, index & 1
        spot = (q, zh, p)
        ids = iter(range(100))

        columns = weights[2].reshape(2, 100, 4, 256).transpose(2, 0, 1, 3)
        part = lambda n: lax.dynamic_index_in_dim(columns, n ^ p, 0, False)
        h0, dh = x[0], dy[0]
        a0 = normed(h0)
        own_g, own_u = weights[0][1], weights[1][1]
        g0, u0, t1, t2, t3, *along = only(
            [
                wide_gather(weights[0][0], X, Y, [0, 2, 4, 6]),
                wide_gather(weights[1][0], Y, X, [1, 3, 5, 7]),
                Swap(*[(part(n), n) for n in (1, 2, 3)], step=1),
                Swap(*[(w, 2 * n) for w in (own_g, own_u) for n in (1, 2, 3)], step=3),
            ],
            next(ids), "fetch",
        )
        ordered = lambda parts, me: jnp.stack([lax.dynamic_index_in_dim(jnp.stack(parts), n ^ me, 0, False) for n in range(len(parts))])
        line_g, line_u = ordered([own_g, *along[:3]], z), ordered([own_u, *along[3:]], z)
        stacked = jnp.stack([part(0), t1, t2, t3])
        turned_down = jnp.concatenate([lax.dynamic_index_in_dim(stacked, n ^ p, 0, False) for n in range(4)], 1)

        at = jnp.arange(D)
        k, r, j, i = at >> 9, (at >> 7) & 3, (at >> 5) & 3, at & 31
        source = (r ^ q) * 256 + (j ^ z) * 64 + (k ^ c) * 32 + i
        order = (source[:, None] == jnp.arange(D)[None, :]).astype(BF)
        turned = lambda a: jnp.einsum("pk,tk->pt", order, a, preferred_element_type=F32).astype(BF)

        act0, s0, t0, d0, gx, gy, gc, uy, ux, uc, other_d = gate_up(
            a0, [g0], [u0],
            [
                down_gather(turned_down[0], X, Y, [0, 4, 9, 16, 19]),
                Halves(line_g, X, Y, [0, 10]),
                Swap((line_u, Y), (line_u, X), (line_u, C), step=11),
                Swap((turned_down[1], ZH), step=10),
            ],
            next(ids),
        )
        h1, a1, g3, gxc, gyc, g3c, u3, uyc, uxc, u3c = down(
            act0, h0, d0, [Finish({X: gx, Y: gy}, X, Y, [0, 7]), Finish({X: ux, Y: uy}, Y, X, [0, 7])], next(ids)
        )
        g1 = [line_g, gc, gy, gyc, gx, gxc, g3, g3c]
        u1 = [line_u, uc, uy, uyc, ux, uxc, u3, u3c]
        at0, at1 = turned(a0), turned(a1)
        act1, s1, t1, d1 = gate_up(a1, g1, u1, [down_gather(ordered([turned_down[1], other_d], zh), Y, X, [0, 5, 12, 18])], next(ids))

        def under(kernel, *args, n, during, name=None):
            pairs = [send() for send, _ in during]
            flat = [pair for some in pairs for pair in some]
            comms = [Swap(*flat)] if flat else []
            out = list(kernel(*args, comms, next(ids)) if name is None else only(comms, next(ids), name))
            at = n
            for some, (_, give) in zip(pairs, during):
                give(*out[at : at + len(some)])
                at += len(some)
            return out[:n]

        lows = {}

        def low(one, n):
            def got(a):
                lows.setdefault(one, []).append(a)
                if n:
                    one.got_low(*lows[one])

            return (lambda: one.low(n)), got

        go = lambda one, name: (getattr(one, name), getattr(one, "got_" + name))
        D1 = DownSum(under(by_down, act1, dh, n=4, during=[]), spot)
        dg, du = under(by_hidden, dh, s1, t1, d1, n=2, during=[go(D1, "core")])
        G1 = WideSum(*under(by_wide, at1, dg, n=2, during=[low(D1, 0)]))
        U1 = WideSum(*under(by_wide, at1, du, n=2, during=[low(D1, 1), go(G1, "core")]))
        (dh,) = under(by_input, dg, du, dh, h1, g1, u1, n=1, during=[go(G1, "axis"), go(U1, "core"), go(D1, "axis")])
        D0 = DownSum(under(by_down, act0, dh, n=4, during=[go(G1, "other"), go(U1, "axis")]), spot)
        dg, du = under(by_hidden, dh, s0, t0, d0, n=2, during=[go(D0, "core"), go(G1, "z"), go(U1, "other"), go(D1, "other")])
        G0 = WideSum(*under(by_wide, at0, dg, n=2, during=[low(D0, 0), go(D1, "high")]))
        U0 = WideSum(*under(by_wide, at0, du, n=2, during=[low(D0, 1), go(D1, "rows")]))
        pair = jnp.stack([jnp.stack([D0.pair(r, side) for side in range(2)]) for r in range(4)])
        G0.sum, U0.sum, block, *rest = tail((G0, U0), pair, U1.z(), next(ids))
        U1.got_z(*rest)
        D0.block = block.reshape(4, 100, 256)
        rows = D0.rows()
        squares = sum(jnp.sum(f32(one) ** 2) for one in (G0.sum, U0.sum, block, G1.sum, U1.sum, D1.sum))
        squares, got = everyone(squares, [a for a, _ in rows], next(ids))
        D0.got_rows(*got)
        sums = [[f32(one.sum) for one in layer] for layer in ((G0, U0, D0), (G1, U1, D1))]
        factor = jnp.minimum(1.0, 0.5 * lax.rsqrt(squares / (6 * D * F) + 1e-30))
        new = []
        for i in range(3):
            g = jnp.stack([sums[0][i], sums[1][i]]) * factor
            new.append(adamw(weights[i].astype(F32), m[i], v[i], g))
        return tuple(one[which] for which in range(3) for one in new)

    states, cut = P(("rep", "dp"), None, None), P(None, "dp", None)
    return jax.shard_map(
        step,
        mesh=mesh,
        in_specs=(states, states) + (cut,) * 9,
        out_specs=(P("rep", "dp", None),) * 9,
        check_vma=False,
    )
```

```python
import jax
import jax.numpy as jnp
from jax import lax
from jax.experimental import pallas as pl
from jax.experimental.pallas import tpu as pltpu
from jax.sharding import PartitionSpec as P

T, D, F = 2048, 1024, 3200
BF, F32 = jnp.bfloat16, jnp.float32
ANY = pl.BlockSpec(memory_space=pl.ANY)
NT = (((1,), (1,)), ((), ()))
TN = (((0,), (0,)), ((), ()))

X, Y, ZH, ZL, C = 16, 8, 4, 2, 1
R = {X: 2, Y: 1}


def normed(h):
    wide = h.astype(F32)
    scale = lax.rsqrt(jnp.mean(wide**2, -1, keepdims=True) + 1e-6)
    return (wide * scale).astype(BF)


def cost(flops, moved, trans=0):
    return pl.CostEstimate(flops=flops, bytes_accessed=moved, transcendentals=trans)


def peer(bits):
    index = lax.axis_index("dp")
    there = index
    for bit in (X, Y, ZH, ZL, C):
        if bits & bit:
            there = there + bit - 2 * bit * ((index // bit) % 2)
    return there


def at_peer(bits, low, high):
    return (peer(bits) // low) % (2 * high // low)


class Gather:
    def __init__(self, own, shape, rounds, steps, home):
        self.home = home
        self.ins, self.outs, self.rounds, self.steps = [own], [jax.ShapeDtypeStruct(shape, BF)], rounds, steps
        self.scratch = [pltpu.VMEM(own.shape, BF), pltpu.SemaphoreType.DMA]

    def place(self, ins, outs, scratch):
        staged, sem = scratch
        dst = self.home(outs[0])
        for pair in ((ins[0], staged), (staged, dst)):
            copy = pltpu.make_async_copy(*pair, sem)
            copy.start()
            copy.wait()


def wide_gather(own, first, second, steps):
    a, b = R[first], R[second]

    def rounds(ins, outs):
        (own,), (buf,) = ins, outs
        part = lambda r, k: buf.at[r, k]
        here = at_peer(0, ZL, ZH)
        there = [at_peer(2 * j, ZL, ZH) for j in (1, 2, 3)]
        over = lambda r, bit: [(buf.at[0, 0, j], buf.at[r, 0, j], bit) for j in there]
        return [
            [(own, buf.at[0, 0, here], 2 * j) for j in (1, 2, 3)] + [(own, buf.at[a, 0, here], first), (own, buf.at[b, 0, here], second)],
            over(a, first) + over(b, second) + [(part(0, 0), part(0, 1), C)],
            [(part(a, 0), part(3, 0), second), (part(a, 0), part(a, 1), C), (part(b, 0), part(b, 1), C)],
            [(part(3, 0), part(3, 1), C)],
        ]

    return Gather(own, (4, 2, 4, 32, F), rounds, steps, lambda buf: buf.at[0, 0, at_peer(0, ZL, ZH)])


def down_gather(own, first, second, steps):
    lined = len(own.shape) == 3
    a, b = R[first], R[second]

    def rounds(ins, outs):
        (own,), (buf,) = ins, outs
        part = lambda l, k, r: buf.at[l, k, r]
        across = lambda l, *rs: [(part(l, 0, r), part(l, 1, r), C) for r in rs]
        over = lambda *rs: [(part(0, 0, r), part(1, 0, r), ZL) for r in rs]
        start = [] if lined else [[(own, buf.at[0, 0, 0, at_peer(0, ZH, ZH)], ZH)]]
        return start + [
            [(part(0, 0, 0), part(0, 0, a), first), (part(0, 0, 0), part(0, 0, b), second)] + over(0) + across(0, 0),
            [(part(0, 0, a), part(0, 0, 3), second)] + over(a, b) + across(0, a, b) + across(1, 0),
            over(3) + across(0, 3) + across(1, a, b),
            across(1, 3),
        ]

    return Gather(own, (2, 2, 4, 2, 400, 256), rounds, steps, lambda buf: buf.at[0, 0, 0] if lined else buf.at[0, 0, 0, at_peer(0, ZH, ZH)])


class Swap:
    def __init__(self, *pairs, step=0):
        self.ins = [a for a, _ in pairs]
        self.outs = [jax.ShapeDtypeStruct(a.shape, a.dtype) for a in self.ins]
        self.rounds = lambda ins, outs: [[(s, d, bits) for s, d, (_, bits) in zip(ins, outs, pairs)]]
        self.steps, self.scratch = [step], []

    def place(self, ins, outs, scratch):
        pass


class Halves(Swap):
    def __init__(self, line, first, second, steps):
        self.ins, self.steps, self.scratch = [line], steps, []
        self.outs = [jax.ShapeDtypeStruct(line.shape, BF)] * 3
        self.rounds = lambda i, o: [
            [(i[0].at[:2], o[0].at[:2], first), (i[0].at[:2], o[1].at[:2], second)],
            [(i[0].at[2:], o[0].at[2:], first), (i[0].at[2:], o[1].at[2:], second), (i[0], o[2], C)],
        ]


def wide_half(own, first, second, steps):
    def rounds(ins, outs):
        (own,), (line, a, b, k) = ins, outs
        return [[(own, line.at[at_peer(0, ZL, ZH)], 2 * j) for j in (1, 2, 3)], [(line, a, first), (line, b, second), (line, k, C)]]

    half = Gather(own, (4, 32, F), rounds, steps, lambda line: line.at[at_peer(0, ZL, ZH)])
    half.outs = half.outs * 4
    return half


class Finish(Swap):
    def __init__(self, parts, first, second, steps):
        self.ins, self.steps, self.scratch = [parts[first], parts[second]], steps, []
        self.outs = [jax.ShapeDtypeStruct((4, 32, F), BF)] * 4
        self.rounds = lambda i, o: [[(i[0], o[0], second), (i[0], o[1], C), (i[1], o[2], C)], [(o[0], o[3], C)]]


def run(body, comms, *, grid, ins, in_specs, outs, out_specs, scratch, number, name, estimate=None):
    n_in, n_out, n_scratch = len(ins), len(outs), len(scratch)
    counts = [(len(c.ins), len(c.outs), len(c.scratch)) for c in comms]
    total = 1
    for n in grid:
        total *= n

    def take(refs, which, start):
        found, at = [], start
        for count in counts:
            found.append(refs[at : at + count[which]])
            at += count[which]
        return found, at

    def kernel(*refs):
        mine_in = refs[:n_in]
        their_ins, at = take(refs, 0, n_in)
        mine_out, at = refs[at : at + n_out], at + n_out
        their_outs, at = take(refs, 1, at)
        mine_scratch, at = refs[at : at + n_scratch], at + n_scratch
        their_scratch, at = take(refs, 2, at)
        send, recv = refs[at:] if comms else (None, None)
        copies, used, bits = [], 0, []
        for c, i, o in zip(comms, their_ins, their_outs):
            per = []
            for one in c.rounds(i, o):
                here = []
                for source, target, b in one:
                    here.append((source, target, b, used))
                    used += 1
                    if b not in bits:
                        bits.append(b)
                per.append(here)
            copies.append(per)

        def make(item):
            source, target, b, n = item
            return pltpu.make_async_remote_copy(
                src_ref=source, dst_ref=target, send_sem=send.at[n], recv_sem=recv.at[n],
                device_id={"dp": peer(b)}, device_id_type=pl.DeviceIdType.MESH,
            )

        events = sorted((s, n, p) for p, c in enumerate(comms) for n, s in enumerate(c.steps))
        if not grid:
            step = 0
        else:
            step = pl.program_id(0)
            for d in range(1, len(grid)):
                step = step * grid[d] + pl.program_id(d)

        def enter():
            barrier = pltpu.get_barrier_semaphore()
            for b in bits:
                pl.semaphore_signal(barrier, inc=1, device_id={"dp": peer(b)}, device_id_type=pl.DeviceIdType.MESH)
            for c, i, o, s in zip(comms, their_ins, their_outs, their_scratch):
                c.place(i, o, s)
            pl.semaphore_wait(barrier, len(bits))

        def advance(now):
            for s, n, p in events:
                if s == now:
                    if n:
                        for item in copies[p][n - 1]:
                            make(item).wait()
                    for item in copies[p][n]:
                        make(item).start()

        def leave():
            for p, c in enumerate(comms):
                for item in copies[p][-1]:
                    make(item).wait()

        if not comms:
            return body(mine_in, mine_out, mine_scratch)
        times = sorted({s for s, _, _ in events})
        if not grid:
            enter()
            for t in times:
                advance(t)
            leave()
            return
        for t in times:

            @pl.when(step == t)
            def _():
                if t == 0:
                    enter()
                advance(t)

        body(mine_in, mine_out, mine_scratch)

        @pl.when(step == total - 1)
        def _():
            leave()

    n_copies = 0
    for c in comms:
        fake = lambda shapes: [Shape(s.shape) for s in shapes]
        n_copies += sum(len(one) for one in c.rounds(fake(c.ins), fake(c.outs)))
    all_scratch = list(scratch) + [s for c in comms for s in c.scratch]
    if comms:
        all_scratch += [pltpu.SemaphoreType.DMA((n_copies,))] * 2
    n_comm_in, n_comm_out = sum(c[0] for c in counts), sum(c[1] for c in counts)
    call = pl.pallas_call(
        kernel,
        grid=grid,
        in_specs=list(in_specs) + [ANY] * n_comm_in,
        out_specs=list(out_specs) + [ANY] * n_comm_out,
        out_shape=list(outs) + [s for c in comms for s in c.outs],
        scratch_shapes=all_scratch,
        compiler_params=pltpu.CompilerParams(collective_id=number, has_side_effects=True) if comms else pltpu.CompilerParams(),
        cost_estimate=estimate,
        name=name,
    )
    return call, (*ins, *[a for c in comms for a in c.ins])


class Shape:
    def __init__(self, shape):
        self.shape, self.at = shape, self

    def __getitem__(self, _):
        return self


def wide_copies(pieces, slot, sem, columns, place):
    for r in range(4):
        for k in range(2):
            piece = pieces[2 * r + k] if len(pieces) == 8 else pieces[0].at[r, k]
            yield pltpu.make_async_copy(piece.at[:, :, columns], slot.at[at_peer(r * Y, Y, X), :, at_peer(k, C, C), :, place], sem)


def down_copies(pieces, slot, sem):
    for l in range(2):
        for k in range(2):
            columns = pl.ds(pl.multiple_of(at_peer(l * ZL + k, C, ZL) * 256, 256), 256)
            for r in range(4):
                yield pltpu.make_async_copy(pieces.at[l, k, r], slot.at[at_peer(r * Y, Y, X), :, :, columns], sem)


def struct(shape, dtype=BF):
    return jax.ShapeDtypeStruct(shape, dtype)


def gate_up(a, gate_w, up_w, comms, number):
    blocks, chunks, rows = 5, 5, 512

    def body(ins, outs, scratch):
        a_ref, *w_refs = ins
        g_ref, u_ref = w_refs[: len(gate_w)], w_refs[len(gate_w) :]
        act_ref, s_ref, t_ref = outs
        slots, sems = scratch
        n, m = pl.program_id(0), pl.program_id(1)

        def copies(block, slot):
            start = pl.multiple_of(block * chunks * 128, 128)
            for k, pieces in enumerate((g_ref, u_ref)):
                yield from wide_copies(pieces, slots.at[slot, k], sems.at[slot], pl.ds(start, chunks * 128), slice(None))

        now = n % 2

        @pl.when((n == 0) & (m == 0))
        def _():
            for copy in copies(0, 0):
                copy.start()

        @pl.when(m == 0)
        def _():
            for copy in copies(n, now):
                copy.wait()

            @pl.when(n + 1 < blocks)
            def _():
                for copy in copies(n + 1, 1 - now):
                    copy.start()

        lhs = a_ref[...]
        for i in range(chunks):
            w = jnp.concatenate([slots[now, k, :, :, :, :, i * 128 : i * 128 + 128].reshape(D, 128) for k in range(2)], 1)
            both = jnp.dot(lhs, w, preferred_element_type=F32)
            gate, up = both[:, :128], both[:, 128:]
            sig = 1.0 / (1.0 + jnp.exp(-gate))
            s = gate * sig
            at = slice(i * 128, i * 128 + 128)
            act_ref[:, at] = (s * up).astype(BF)
            s_ref[:, at] = s
            t_ref[:, at] = up * (sig + s * (1.0 - sig))

    out = pl.BlockSpec((rows, chunks * 128), lambda n, m: (m, n))
    call, operands = run(
        body, comms, grid=(blocks, T // rows),
        ins=[a, *gate_w, *up_w], in_specs=[pl.BlockSpec((rows, D), lambda n, m: (m, 0))] + [ANY] * len(gate_w + up_w),
        outs=[struct((T, F)), struct((T, F), F32), struct((T, F), F32)], out_specs=[out] * 3,
        scratch=[pltpu.VMEM((2, 2, 4, 4, 2, 32, chunks * 128), BF), pltpu.SemaphoreType.DMA((2,))],
        number=number, name="gate_up", estimate=cost(4 * T * D * F, T * F * 10 + 4 * D * F, T * F * 2),
    )
    return call(*operands)


def row(rows, n):
    return pl.BlockSpec((rows, n), lambda m: (m, 0))


def fetch_down(p_ref, w_ref, sem):
    @pl.when(pl.program_id(0) == 0)
    def _():
        for copy in down_copies(p_ref, w_ref, sem):
            copy.start()
        for copy in down_copies(p_ref, w_ref, sem):
            copy.wait()


def down(act, h, pieces, comms, number):
    def body(ins, outs, scratch):
        act_ref, h_ref, p_ref = ins
        fetch_down(p_ref, *scratch)
        out = h_ref[...] + jnp.dot(act_ref[...], scratch[0][...].reshape(F, D), preferred_element_type=F32).astype(BF)
        outs[0][...] = out
        outs[1][...] = normed(out)

    call, operands = run(
        body, comms, grid=(T // 256,), ins=[act, h, pieces], in_specs=[row(256, F), row(256, D), ANY],
        outs=[struct((T, D))] * 2, out_specs=[row(256, D)] * 2, scratch=[pltpu.VMEM((4, 2, 400, D), BF), pltpu.SemaphoreType.DMA],
        number=number, name="down", estimate=cost(2 * T * D * F, T * F * 2 + T * D * 6 + 2 * D * F),
    )
    return call(*operands)


def by_hidden(dh, s, t, pieces, comms, number):
    def body(ins, outs, scratch):
        dh_ref, s_ref, t_ref, p_ref = ins
        dg_ref, du_ref = outs
        w_ref = scratch[0]
        fetch_down(p_ref, *scratch)
        lhs = dh_ref[...]
        w = w_ref[...].reshape(F, D)
        for at in range(0, F, 640):
            at = slice(at, at + 640)
            d = lax.dot_general(lhs, w[at, :], NT, preferred_element_type=F32).astype(BF).astype(F32)
            du_ref[:, at] = (d * s_ref[:, at]).astype(BF)
            dg_ref[:, at] = (d * t_ref[:, at]).astype(BF)

    call, operands = run(
        body, comms, grid=(T // 256,), ins=[dh, s, t, pieces], in_specs=[row(256, D), row(256, F), row(256, F), ANY],
        outs=[struct((T, F))] * 2, out_specs=[row(256, F)] * 2, scratch=[pltpu.VMEM((4, 2, 400, D), BF), pltpu.SemaphoreType.DMA],
        number=number, name="by_hidden", estimate=cost(2 * T * D * F, T * F * 12 + T * D * 2 + 2 * D * F),
    )
    return call(*operands)


def by_input(dg, du, dh, h, gate_w, up_w, comms, number):
    def body(ins, outs, scratch):
        dg_ref, du_ref, dh_ref, h_ref, *w_refs = ins
        g_ref, u_ref = w_refs[: len(gate_w)], w_refs[len(gate_w) :]
        slots, sems = scratch

        @pl.when(pl.program_id(0) == 0)
        def _():
            both = [c for k, p in enumerate((g_ref, u_ref)) for c in wide_copies(p, slots.at[k], sems.at[k], slice(None), slice(None))]
            for copy in both:
                copy.start()
            for copy in both:
                copy.wait()

        halves = []
        for k, d_ref in enumerate((dg_ref, du_ref)):
            w = slots[k].reshape(D, F)
            halves.append(lax.dot_general(d_ref[...], w, NT, preferred_element_type=F32).astype(BF))
        da = (halves[0] + halves[1]).astype(F32)
        wide = h_ref[...].astype(F32)
        scale = lax.rsqrt(jnp.mean(wide**2, -1, keepdims=True) + 1e-6)
        along = jnp.mean(da * wide, -1, keepdims=True)
        outs[0][...] = dh_ref[...] + (da * scale - wide * (scale * scale * scale * along)).astype(BF)

    call, operands = run(
        body, comms, grid=(T // 256,), ins=[dg, du, dh, h, *gate_w, *up_w],
        in_specs=[row(256, F), row(256, F), row(256, D), row(256, D)] + [ANY] * len(gate_w + up_w),
        outs=[struct((T, D))], out_specs=[row(256, D)],
        scratch=[pltpu.VMEM((2, 4, 4, 2, 32, F), BF), pltpu.SemaphoreType.DMA((2,))],
        number=number, name="by_input", estimate=cost(4 * T * D * F, T * F * 4 + T * D * 6 + 4 * D * F),
    )
    return call(*operands)


def by_wide(at, d, comms, number):
    columns = 640

    def body(ins, outs, scratch):
        at_ref, d_ref = ins
        for k, ref in enumerate(outs):
            ref[...] = jnp.dot(at_ref[k * D // 2 : (k + 1) * D // 2, :], d_ref[...], preferred_element_type=F32).astype(BF)

    out = pl.BlockSpec((D // 2, columns), lambda n: (0, n))
    call, operands = run(
        body, comms, grid=(F // columns,), ins=[at, d],
        in_specs=[pl.BlockSpec((D, T), lambda n: (0, 0)), pl.BlockSpec((T, columns), lambda n: (0, n))],
        outs=[struct((D // 2, F))] * 2, out_specs=[out] * 2, scratch=[],
        number=number, name="by_wide", estimate=cost(2 * T * D * F, T * F * 2 + T * D * 2 + D * F * 2),
    )
    return call(*operands)


def by_down(act, dh, comms, number):
    rows = 640

    def body(ins, outs, scratch):
        act_ref, dh_ref = ins
        for n, ref in enumerate(outs):
            columns = pl.ds(pl.multiple_of(at_peer(n, C, ZL) * 256, 256), 256)
            ref[...] = lax.dot_general(act_ref[...], dh_ref[:, columns], TN, preferred_element_type=F32).astype(BF)

    call, operands = run(
        body, comms, grid=(F // rows,), ins=[act, dh],
        in_specs=[pl.BlockSpec((T, rows), lambda n: (0, n)), pl.BlockSpec((T, D), lambda n: (0, 0))],
        outs=[struct((F, 256))] * 4, out_specs=[pl.BlockSpec((rows, 256), lambda n: (n, 0))] * 4, scratch=[],
        number=number, name="by_down", estimate=cost(2 * T * D * F, T * F * 2 + T * D * 2 + D * F * 2),
    )
    return call(*operands)


def only(comms, number, name):
    call, operands = run(None, comms, grid=(), ins=[], in_specs=[], outs=[], out_specs=[], scratch=[], number=number, name=name)
    return call(*operands)


class Copies:
    def __init__(self, send, recv):
        self.send, self.recv, self.n = send, recv, 0

    def __call__(self, source, target, bits):
        copy = pltpu.make_async_remote_copy(
            src_ref=source, dst_ref=target, send_sem=self.send.at[self.n], recv_sem=self.recv.at[self.n],
            device_id={"dp": peer(bits)}, device_id_type=pl.DeviceIdType.MESH,
        )
        copy.start()
        self.n += 1
        return copy


def meet(bits):
    barrier = pltpu.get_barrier_semaphore()
    for b in bits:
        pl.semaphore_signal(barrier, inc=1, device_id={"dp": peer(b)}, device_id_type=pl.DeviceIdType.MESH)
    pl.semaphore_wait(barrier, len(bits))


VMEM = pl.BlockSpec(memory_space=pltpu.VMEM)


def everyone(value, pieces, number):
    groups = (tuple(range(1, 8)), (8, 16, 24))

    def kernel(value_ref, p1, p2, p3, out_ref, o1, o2, o3, mid_ref, slots, send, recv):
        meet(groups[0] + groups[1])
        begin = Copies(send, recv)
        source, target, n = value_ref, mid_ref, 0
        rest = []
        for group in groups:
            copies = [begin(source, slots.at[n + i], b) for i, b in enumerate(group)]
            if not rest:
                rest = [begin(a, b, bits) for a, b, bits in ((p1, o1, 1), (p2, o2, 2), (p3, o3, 3))]
            total = source[...]
            for copy in copies:
                copy.wait()
                total = total + slots[n]
                n += 1
            target[...] = total
            source, target = mid_ref, out_ref
        for copy in rest:
            copy.wait()

    call = pl.pallas_call(
        kernel, in_specs=[VMEM] + [ANY] * 3, out_specs=[VMEM] + [ANY] * 3,
        out_shape=[struct((8, 128), F32)] + [struct(a.shape) for a in pieces],
        scratch_shapes=[pltpu.VMEM((8, 128), F32), pltpu.VMEM((10, 8, 128), F32)] + [pltpu.SemaphoreType.DMA((13,))] * 2,
        compiler_params=pltpu.CompilerParams(collective_id=number, has_side_effects=True), name="everyone",
    )
    total, *got = call(jnp.broadcast_to(value, (8, 128)), *pieces)
    return total[0, 0], got


def tail(wides, pair, swaps, number):
    n, width, ns = 5, 640, len(swaps)
    ways = ((X, Y), (Y, X))

    def kernel(*refs):
        keeps, sends, pd = refs[:2], refs[2:4], refs[4]
        swap_in, refs = refs[5 : 5 + ns], refs[5 + ns :]
        outs, out_d, swap_out, refs = refs[:2], refs[2], refs[3 : 3 + ns], refs[3 + ns :]
        got, snd1, rcv1, snd2, rcv2, tot, snd3, rcv3, sd1, rd1, sd2, rd2, td, sd3, rd3, send, recv = refs
        begin = Copies(send, recv)
        at = lambda u: slice(u * width, (u + 1) * width)
        meet((C, X, Y, 2, 4, 6))
        core = [[begin(sends[w].at[:, at(u)], got.at[w, u], C) for w in range(2)] for u in range(n)]
        others = [begin(a, b, bits) for a, b, (_, bits) in zip(swap_in, swap_out, swaps)]
        first, second, last, down1, down2, down3 = {}, {}, {}, {}, {}, []

        def term(w, u, r):
            rows = slice(r * 128, r * 128 + 128)
            return f32(keeps[w][rows, at(u)]) + f32(got[w, u, rows, :])

        def axis(u):
            for w, (one, _) in enumerate(ways):
                core[u][w].wait()
                snd1[w, u, 0] = term(w, u, 3).astype(BF)
                snd1[w, u, 1] = term(w, u, R[one]).astype(BF)
            for i in range(2):
                for w, (one, _) in enumerate(ways):
                    first[w, u, i] = begin(snd1.at[w, u, i], rcv1.at[w, u, i], one)

        def other(u):
            for w, (_, two) in enumerate(ways):
                first[w, u, 0].wait()
                snd2[w, u] = (term(w, u, R[two]) + f32(rcv1[w, u, 0])).astype(BF)
            for w, (_, two) in enumerate(ways):
                second[w, u] = begin(snd2.at[w, u], rcv2.at[w, u], two)

        def line(u):
            for w in range(2):
                first[w, u, 1].wait()
                second[w, u].wait()
                total = term(w, u, 0) + f32(rcv1[w, u, 1]) + f32(rcv2[w, u])
                tot[w, u] = total[:32]
                for j in (1, 2, 3):
                    snd3[w, u, j - 1] = total[32 * j : 32 * j + 32].astype(BF)
            for w in range(2):
                last[w, u] = [begin(snd3.at[w, u, j - 1], rcv3.at[w, u, j - 1], 2 * j) for j in (1, 2, 3)]

        def end(u):
            for w in range(2):
                total = tot[w, u]
                for i, copy in enumerate(last[w, u]):
                    copy.wait()
                    total = total + f32(rcv3[w, u, i])
                outs[w][:, at(u)] = total.astype(BF)

        def down_axis():
            for w, (one, _) in enumerate(ways):
                sd1[w, 0] = pd[3, w].astype(BF)
                sd1[w, 1] = pd[R[one], w].astype(BF)
            for w, (one, _) in enumerate(ways):
                down1[w] = [begin(sd1.at[w, i], rd1.at[w, i], one) for i in range(2)]

        def down_other():
            for w, (_, two) in enumerate(ways):
                down1[w][0].wait()
                sd2[w] = (pd[R[two], w] + f32(rd1[w, 0])).astype(BF)
            for w, (_, two) in enumerate(ways):
                down2[w] = begin(sd2.at[w], rd2.at[w], two)

        def down_line():
            for w in range(2):
                down1[w][1].wait()
                down2[w].wait()
                td[w] = pd[0, w] + f32(rd1[w, 1]) + f32(rd2[w])
            sd3[...] = td[at_peer(ZH, ZH, ZH)].astype(BF)
            down3.append(begin(sd3, rd3, ZH))

        for s in range(n + 3):
            if s < n:
                axis(s)
            if s == 1:
                down_axis()
            if 0 <= s - 1 < n:
                other(s - 1)
            if s == 3:
                down_other()
            if 0 <= s - 2 < n:
                line(s - 2)
            if s == 4:
                down_line()
            if 0 <= s - 3 < n:
                end(s - 3)
        down3[0].wait()
        out_d[...] = (td[at_peer(0, ZH, ZH)] + f32(rd3[...])).astype(BF)
        for copy in others:
            copy.wait()

    vm = lambda *shape: pltpu.VMEM(shape, BF)
    total = n * 2 * 7 + 7 + ns
    call = pl.pallas_call(
        kernel, in_specs=[VMEM] * 2 + [ANY] * 2 + [VMEM] + [ANY] * ns, out_specs=[VMEM] * 3 + [ANY] * ns,
        out_shape=[struct((32, F))] * 2 + [struct((400, 256))] + [struct(a.shape) for a, _ in swaps],
        scratch_shapes=[
            vm(2, n, 512, width), vm(2, n, 2, 128, width), vm(2, n, 2, 128, width), vm(2, n, 128, width), vm(2, n, 128, width),
            pltpu.VMEM((2, n, 32, width), F32), vm(2, n, 3, 32, width), vm(2, n, 3, 32, width),
            vm(2, 2, 400, 256), vm(2, 2, 400, 256), vm(2, 400, 256), vm(2, 400, 256), pltpu.VMEM((2, 400, 256), F32), vm(400, 256), vm(400, 256),
        ] + [pltpu.SemaphoreType.DMA((total,))] * 2,
        compiler_params=pltpu.CompilerParams(collective_id=number, has_side_effects=True), name="tail",
    )
    return call(*[w.keep.reshape(512, F) for w in wides], *[w.send.reshape(512, F) for w in wides], pair, *[a for a, _ in swaps])


def adamw(w, m, v, g):
    m = 0.9 * m + 0.1 * g
    v = 0.95 * v + 0.05 * g * g
    step = m * lax.rsqrt(v + 1e-8) + 0.1 * w
    return (w - 0.02 * step).astype(BF), m, v


def f32(a):
    return a.astype(F32)


LEFT, RIGHT = slice(0, 1664), slice(1664, F)


class WideSum:
    def __init__(self, keep, send):
        self.keep, self.send = keep.reshape(4, 4, 32, F), send.reshape(4, 4, 32, F)

    def core(self):
        return [(self.send, C)]

    def got_core(self, got):
        self.pair = lambda r, columns: f32(self.keep[r][..., columns]) + f32(got[r][..., columns])

    def axis(self):
        one = lambda r, columns: self.pair(r, columns).astype(BF)
        return [(one(3, LEFT), X), (one(2, LEFT), X), (one(3, RIGHT), Y), (one(1, RIGHT), Y)]

    def got_axis(self, *got):
        self.got = got

    def other(self):
        return [((self.pair(1, LEFT) + f32(self.got[0])).astype(BF), Y), ((self.pair(2, RIGHT) + f32(self.got[2])).astype(BF), X)]

    def got_other(self, left, right):
        self.left = self.pair(0, LEFT) + f32(self.got[1]) + f32(left)
        self.right = self.pair(0, RIGHT) + f32(self.got[3]) + f32(right)

    def z(self):
        return [(side[j].astype(BF), 2 * j) for side in (self.left, self.right) for j in (1, 2, 3)]

    def got_z(self, *rest):
        total = lambda side, some: (side[0] + sum(f32(r) for r in some)).astype(BF)
        self.sum = jnp.concatenate([total(self.left, rest[:3]), total(self.right, rest[3:])], 1)


class DownSum:
    def __init__(self, parts, spot):
        self.parts, self.spot = parts, spot

    def core(self):
        return [(self.parts[1], C), (self.parts[3], C)]

    def got_core(self, mine, low):
        self.mine = mine
        self.to_low = (f32(self.parts[2]) + f32(low)).astype(BF).reshape(2, 1600, 256)

    def low(self, n):
        return [(self.to_low[n], ZL)]

    def got_low(self, *got):
        q = self.spot[0]
        quarters = lambda a: a.reshape(4, 2, 400, 256)
        pick = lambda a, r, side: f32(lax.dynamic_index_in_dim(quarters(a), r ^ q, 0, False)[side])

        def lows(r, side):
            both = [g.reshape(2, 2, 400, 256) for g in got]
            at = r ^ q
            return f32(jnp.where(at < 2, *[lax.dynamic_index_in_dim(b, at & 1, 0, False)[side] for b in both]))

        self.pair = lambda r, side: pick(self.parts[0], r, side) + pick(self.mine, r, side) + lows(r, side)

    def axis(self):
        one = lambda r, side: self.pair(r, side).astype(BF)
        return [(one(3, 0), X), (one(2, 0), X), (one(3, 1), Y), (one(1, 1), Y)]

    def got_axis(self, *got):
        self.got = got

    def other(self):
        return [((self.pair(1, 0) + f32(self.got[0])).astype(BF), Y), ((self.pair(2, 1) + f32(self.got[2])).astype(BF), X)]

    def got_other(self, first, second):
        total = jnp.stack([self.pair(0, 0) + f32(self.got[1]) + f32(first), self.pair(0, 1) + f32(self.got[3]) + f32(second)])
        self.half = lambda h: lax.dynamic_index_in_dim(total, h ^ self.spot[1], 0, False)

    def high(self):
        return [(self.half(1).astype(BF), ZH)]

    def got_high(self, got):
        self.block = (self.half(0) + f32(got)).astype(BF).reshape(4, 100, 256)

    def rows(self):
        pick = lambda n: lax.dynamic_index_in_dim(self.block, n ^ self.spot[2], 0, False)
        self.own = pick(0)
        return [(pick(n), n) for n in (1, 2, 3)]

    def got_rows(self, *rest):
        stacked = jnp.stack((self.own,) + rest)
        self.sum = jnp.concatenate([lax.dynamic_index_in_dim(stacked, n ^ self.spot[2], 0, False) for n in range(4)], 1)


def solution(mesh):
    def step(x, dy, *arrays):
        weights, m, v = (arrays[i : i + 3] for i in (0, 3, 6))
        index = lax.axis_index("dp")
        q, zh, p = index >> 3, (index >> 2) & 1, index & 3
        z, c = (index >> 1) & 3, index & 1
        spot = (q, zh, p)
        ids = iter(range(100))

        columns = weights[2].reshape(2, 100, 4, 256).transpose(2, 0, 1, 3)
        part = lambda n: lax.dynamic_index_in_dim(columns, n ^ p, 0, False)
        h0, dh = x[0], dy[0]
        a0 = normed(h0)
        own_g, own_u = weights[0][1], weights[1][1]
        g0, u0, t1, t2, t3, *along = only(
            [
                wide_gather(weights[0][0], X, Y, [0, 2, 4, 6]),
                wide_gather(weights[1][0], Y, X, [1, 3, 5, 7]),
                Swap(*[(part(n), n) for n in (1, 2, 3)], step=1),
                Swap(*[(own_g, 2 * n) for n in (1, 2, 3)], step=3),
            ],
            next(ids), "fetch",
        )
        ordered = lambda parts, me: jnp.stack([lax.dynamic_index_in_dim(jnp.stack(parts), n ^ me, 0, False) for n in range(len(parts))])
        line_g = ordered([own_g, *along], z)
        stacked = jnp.stack([part(0), t1, t2, t3])
        turned_down = jnp.concatenate([lax.dynamic_index_in_dim(stacked, n ^ p, 0, False) for n in range(4)], 1)

        at = jnp.arange(D)
        k, r, j, i = at >> 9, (at >> 7) & 3, (at >> 5) & 3, at & 31
        source = (r ^ q) * 256 + (j ^ z) * 64 + (k ^ c) * 32 + i
        order = (source[:, None] == jnp.arange(D)[None, :]).astype(BF)
        turned = lambda a: jnp.einsum("pk,tk->pt", order, a, preferred_element_type=F32).astype(BF)

        act0, s0, t0, d0, gx, gy, gc, line_u, uy, ux, uc, other_d = gate_up(
            a0, [g0], [u0],
            [
                down_gather(turned_down[0], X, Y, [0, 4, 9, 16, 19]),
                Halves(line_g, X, Y, [0, 10]),
                wide_half(own_u, Y, X, [3, 12]),
                Swap((turned_down[1], ZH), step=10),
            ],
            next(ids),
        )
        h1, a1, g3, gxc, gyc, g3c, u3, uyc, uxc, u3c = down(
            act0, h0, d0, [Finish({X: gx, Y: gy}, X, Y, [0, 7]), Finish({X: ux, Y: uy}, Y, X, [0, 7])], next(ids)
        )
        g1 = [line_g, gc, gy, gyc, gx, gxc, g3, g3c]
        u1 = [line_u, uc, uy, uyc, ux, uxc, u3, u3c]
        at0, at1 = turned(a0), turned(a1)
        act1, s1, t1, d1 = gate_up(a1, g1, u1, [down_gather(ordered([turned_down[1], other_d], zh), Y, X, [0, 5, 12, 18])], next(ids))

        def under(kernel, *args, n, during, name=None):
            pairs = [send() for send, _ in during]
            flat = [pair for some in pairs for pair in some]
            comms = [Swap(*flat)] if flat else []
            out = list(kernel(*args, comms, next(ids)) if name is None else only(comms, next(ids), name))
            at = n
            for some, (_, give) in zip(pairs, during):
                give(*out[at : at + len(some)])
                at += len(some)
            return out[:n]

        lows = {}

        def low(one, n):
            def got(a):
                lows.setdefault(one, []).append(a)
                if n:
                    one.got_low(*lows[one])

            return (lambda: one.low(n)), got

        go = lambda one, name: (getattr(one, name), getattr(one, "got_" + name))
        D1 = DownSum(under(by_down, act1, dh, n=4, during=[]), spot)
        dg, du = under(by_hidden, dh, s1, t1, d1, n=2, during=[go(D1, "core")])
        G1 = WideSum(*under(by_wide, at1, dg, n=2, during=[low(D1, 0)]))
        U1 = WideSum(*under(by_wide, at1, du, n=2, during=[low(D1, 1), go(G1, "core")]))
        (dh,) = under(by_input, dg, du, dh, h1, g1, u1, n=1, during=[go(G1, "axis"), go(U1, "core"), go(D1, "axis")])
        D0 = DownSum(under(by_down, act0, dh, n=4, during=[go(G1, "other"), go(U1, "axis")]), spot)
        dg, du = under(by_hidden, dh, s0, t0, d0, n=2, during=[go(D0, "core"), go(G1, "z"), go(U1, "other"), go(D1, "other")])
        G0 = WideSum(*under(by_wide, at0, dg, n=2, during=[low(D0, 0), go(D1, "high")]))
        U0 = WideSum(*under(by_wide, at0, du, n=2, during=[low(D0, 1), go(D1, "rows")]))
        pair = jnp.stack([jnp.stack([D0.pair(r, side) for side in range(2)]) for r in range(4)])
        G0.sum, U0.sum, block, *rest = tail((G0, U0), pair, U1.z(), next(ids))
        U1.got_z(*rest)
        D0.block = block.reshape(4, 100, 256)
        rows = D0.rows()
        squares = sum(jnp.sum(f32(one) ** 2) for one in (G0.sum, U0.sum, block, G1.sum, U1.sum, D1.sum))
        squares, got = everyone(squares, [a for a, _ in rows], next(ids))
        D0.got_rows(*got)
        sums = [[f32(one.sum) for one in layer] for layer in ((G0, U0, D0), (G1, U1, D1))]
        factor = jnp.minimum(1.0, 0.5 * lax.rsqrt(squares / (6 * D * F) + 1e-30))
        new = []
        for i in range(3):
            g = jnp.stack([sums[0][i], sums[1][i]]) * factor
            new.append(adamw(weights[i].astype(F32), m[i], v[i], g))
        return tuple(one[which] for which in range(3) for one in new)

    states, cut = P(("rep", "dp"), None, None), P(None, "dp", None)
    return jax.shard_map(
        step,
        mesh=mesh,
        in_specs=(states, states) + (cut,) * 9,
        out_specs=(P("rep", "dp", None),) * 9,
        check_vma=False,
    )
```
